256 devices in a mesh: stat: 32 (over x_hi, z, core), tm: 8 (over y, x_lo).
Axes of the slice: x: 4 (x_hi: 2, x_lo: 2; x = x_hi * 2 + x_lo), y: 4, z: 8, core: 2. Of those that a mesh axis runs over, the one named last changes fastest.
Arguments:
- voltages: bfloat16 [2, 1024, 32, 4096], P(None, 'stat', 'tm'), may hold values from -6 to 6
- beam_weights: bfloat16 [2, 1024, 256], P(None, 'stat'), may hold values from -0.125 to 0.125
Outputs:
- beams: bfloat16 [4096, 32, 2, 256], P('stat', 'tm')
- visibilities: float32 [1024, 32, 2, 1024], P('tm', 'stat')
The draws below stay inside these ranges and needn't reach their ends.
All inputs are finite; a program needn't handle non-finite values.
Results may differ from the reference program's by a relative error of at most 0.011.
Values may be sent and summed in bfloat16 or wider, within the bound.
No kernel may reach another device: no remote copies, remote signals or barrier semaphores. Data moves between devices by JAX's collectives and lax.ppermute only.
A program may use at most 64 MiB of HBM per device.

```python
import jax
import jax.numpy as jnp
from jax import lax

INPUTS = 1024
NA = 16
NB = 256
BEAMS = 256
AVG = 128
NF = 4096
SPEC = 32
VCH = 32
N_STAT = 32


def shard_levels(own_key, dims, cuts, low, largest):
    gain = 1.0
    for position, parts in cuts:
        draws = jax.random.uniform(jax.random.fold_in(jax.random.fold_in(own_key, 6), position), (parts,), jnp.float32, low / len(cuts), largest / len(cuts))
        gain = gain * jnp.repeat(jnp.exp(draws), dims[position] // parts).reshape((-1,) + (1,) * (len(dims) - 1 - position))
    return gain


def gaussian(stream_key, dims, scale, limit, shards=(), kind=jnp.bfloat16):
    level = shard_levels(stream_key, dims, shards, -0.22, 0.18) if shards else 1.0
    array = jax.random.normal(stream_key, dims, jnp.float32) * scale * level
    return jnp.minimum(jnp.maximum(array, -limit), limit).astype(kind)


def setup_inputs(seed: int = 0) -> dict:
    arg_keys = jax.random.split(jax.random.key(seed), 3)
    return {
        "voltages": gaussian(arg_keys[0], (2, INPUTS, SPEC, NF), 1.0, 6.0, ((1, 32), (2, 8))),
        "beam_weights": gaussian(arg_keys[1], (2, INPUTS, BEAMS), (2 * INPUTS) ** -0.5, 0.125, ((1, 32),)),
    }


def block_spectra(volt_block):
    signal = volt_block[0].astype(jnp.float32) + 1j * volt_block[1].astype(jnp.float32)
    transform = jnp.fft.fft(signal, axis=-1, norm="ortho")
    return jnp.stack([jnp.real(transform), jnp.imag(transform)]).astype(jnp.bfloat16)


def reference(voltages, beam_weights):
    block_width = INPUTS // N_STAT
    total_channels = NA * NB
    grouped = voltages.reshape(2, N_STAT, block_width, SPEC, total_channels).transpose(1, 0, 2, 3, 4)
    spectra = lax.map(block_spectra, grouped)
    weight_stack = jnp.stack([jnp.stack([beam_weights[0], beam_weights[1]], 1), jnp.stack([-beam_weights[1], beam_weights[0]], 1)], 0)
    weight_blocks = weight_stack.reshape(2, N_STAT, block_width, 2, BEAMS).transpose(1, 0, 2, 3, 4)

    def add_block(running, pair):
        spec_block, weight_block = pair
        partial_value = jnp.einsum('pisc,piqb->csqb', spec_block.astype(jnp.float32), weight_block.astype(jnp.float32))
        rounded = lax.optimization_barrier(partial_value.astype(jnp.bfloat16))
        return running + rounded.astype(jnp.float32), None

    beam_total, _ = lax.scan(add_block, jnp.zeros((total_channels, SPEC, 2, BEAMS), jnp.float32), (spectra, weight_blocks))
    beams = beam_total.astype(jnp.bfloat16)
    all_spectra = spectra.transpose(1, 0, 2, 3, 4).reshape(2, INPUTS, SPEC, total_channels)
    scale = 1.0 / (SPEC * AVG)

    def one_channel(channel_index):
        band = lax.dynamic_slice_in_dim(all_spectra, channel_index * AVG, AVG, 3).astype(jnp.float32)
        real_gram = jnp.einsum('pisc,pjsc->ij', band, band)
        mixed = jnp.einsum('isc,jsc->ij', band[1], band[0])
        return jnp.stack([real_gram, mixed - mixed.T]) * scale

    stacked = lax.map(one_channel, jnp.arange(VCH, dtype=jnp.int32))
    visibilities = stacked.transpose(2, 0, 1, 3)
    return beams, visibilities
```

```python
import math

import jax
import jax.numpy as jnp
import numpy as np
from jax import lax
from jax.experimental import pallas as pl
from jax.experimental.pallas import tpu as pltpu
from jax.sharding import Mesh
from jax.sharding import PartitionSpec as P

STAT = ("stat_0", "stat_1", "stat_2")
TM = ("tm_0", "tm_1")
NF = 4096
N_STAT = 32
N_TM = 8
SPECTRA = 4
CHUNKS = 4
IC = 8
ROWS = N_STAT * IC
OWN = ROWS // N_TM
HALF = 512
BF16 = jnp.bfloat16
F32 = jnp.float32
VMEM = pl.BlockSpec(memory_space=pltpu.VMEM)


def rotation(angle):
    cosine, sine = np.cos(angle), np.sin(angle)
    return np.block([[cosine, sine], [-sine, cosine]])


def dft_tables():
    outer = np.arange(32)
    first = 2.0 * np.pi * np.outer(outer, outer) / 32
    cosine, sine = np.cos(first), np.sin(first)
    eye = np.eye(SPECTRA)
    spread = lambda m: np.einsum("wc,st->wsct", m, eye).reshape(128, 128)
    left = np.block([[spread(cosine), spread(sine)], [-spread(sine), spread(cosine)]])
    w0 = np.repeat(np.arange(32), SPECTRA)
    twist = 2.0 * np.pi * np.outer(w0, np.arange(128)) / NF
    inner = 2.0 * np.pi * np.outer(np.arange(128), np.arange(128)) / 128
    right = rotation(inner) / math.sqrt(NF)
    right = right.reshape(2, 32, 4, 256).transpose(1, 0, 2, 3).reshape(256, 256)
    return (
        left.astype(np.float32),
        np.cos(twist).astype(np.float32),
        np.sin(twist).astype(np.float32),
        right.astype(np.float32),
    )


def natural_order(groups):
    source = np.arange(CHUNKS * groups * 4 * IC).reshape(CHUNKS, groups, 4, IC)
    target = source.transpose(1, 2, 0, 3).reshape(-1)
    order = np.zeros((source.size, source.size), np.float32)
    order[target, np.arange(source.size)] = 1.0
    return order


def params(mib):
    return pltpu.CompilerParams(vmem_limit_bytes=mib * 1024 * 1024)


def cost(macs, moved):
    return pl.CostEstimate(flops=2 * macs, bytes_accessed=moved, transcendentals=0)


def dot_nn(a, b):
    return lax.dot_general(a, b, (((1,), (0,)), ((), ())), preferred_element_type=F32)


def dot_nt(a, b):
    return lax.dot_general(a, b, (((1,), (1,)), ((), ())), preferred_element_type=F32)


def dft_kernel(x_ref, left_ref, cos_ref, sin_ref, right_ref, out_ref, stage):
    left = left_ref[...]
    right = right_ref[...]
    cosine = cos_ref[...]
    sine = sin_ref[...]
    for pair in range(IC // 2):
        signal = [jnp.concatenate([x_ref[0, 2 * pair + k], x_ref[1, 2 * pair + k]], 0) for k in (0, 1)]
        first = dot_nn(left, jnp.concatenate(signal, 1))
        turned = []
        for k in (0, 1):
            re = first[:128, 128 * k : 128 * k + 128]
            im = first[128:, 128 * k : 128 * k + 128]
            turned.append(
                jnp.concatenate(
                    [(re * cosine + im * sine).astype(BF16), (im * cosine - re * sine).astype(BF16)], 1
                )
            )
        final = dot_nt(right, jnp.concatenate(turned, 0))
        for k in (0, 1):
            stage[pl.ds(2 * pair + k, 256, stride=IC), :] = final[:, 128 * k : 128 * k + 128]
    for v in range(N_STAT):
        for t in range(8):
            row = (v * 8 + t) * IC
            out_ref[v, :, 128 * t : 128 * t + 128] = stage[row : row + IC, :].astype(BF16)


def dft_chunk(signal, tables, chunk):
    full = lambda a: pl.BlockSpec(a.shape, lambda i: (0,) * a.ndim)
    return pl.pallas_call(
        dft_kernel,
        grid=(1,),
        in_specs=[pl.BlockSpec((2, IC, 128, 128), lambda i: (0, chunk, 0, 0))] + [full(t) for t in tables],
        out_specs=pl.BlockSpec((N_STAT, IC, 1024), lambda i: (0, 0, 0)),
        out_shape=jax.ShapeDtypeStruct((N_STAT, IC, 1024), BF16),
        scratch_shapes=[pltpu.VMEM((256 * IC, 128), F32)],
        compiler_params=params(10),
        cost_estimate=cost(1 << 28, 1 << 21),
        name=f"dft_{chunk}",
    )(signal, *tables)


def gram_kernel(*refs):
    out_ref = refs[-1]
    chunks = refs[:-1]
    mine = chunks[-1][...]
    scale = 1.0 / NF
    for c, ref in enumerate(chunks):
        other = ref[...]
        real = dot_nt(mine, other) * scale
        imag = (dot_nt(mine[:, HALF:], other[:, :HALF]) - dot_nt(mine[:, :HALF], other[:, HALF:])) * scale
        for r in range(N_TM):
            out_ref[r, 0, :, ROWS * c : ROWS * c + ROWS] = real[OWN * r : OWN * r + OWN].astype(BF16)
            out_ref[r, 1, :, ROWS * c : ROWS * c + ROWS] = imag[OWN * r : OWN * r + OWN].astype(BF16)


def gram(chunks):
    count = len(chunks)
    return pl.pallas_call(
        gram_kernel,
        in_specs=[VMEM] * count,
        out_specs=VMEM,
        out_shape=jax.ShapeDtypeStruct((N_TM, 2, OWN, ROWS * count), BF16),
        compiler_params=params(8),
        cost_estimate=cost(count << 27, count << 20),
        name=f"gram_{count}",
    )(*chunks)


def mirror_kernel(*refs):
    terms, sums_ref, mirror_ref = refs[:CHUNKS], refs[-2], refs[-1]
    for q in (0, 1):
        sums = []
        for c in range(CHUNKS):
            ref = terms[c]
            if len(ref.shape) == 4:
                total = ref[0, q].astype(F32)
                for t in range(1, N_TM):
                    total = total + ref[t, q].astype(F32)
            else:
                total = ref[q]
            sums.append(total)
            width = ROWS * (c + 1)
            sums_ref[q, OWN * c : OWN * c + OWN, :width] = total
            if width < ROWS * CHUNKS:
                sums_ref[q, OWN * c : OWN * c + OWN, width:] = jnp.zeros((OWN, ROWS * CHUNKS - width), F32)
        sign = -1.0 if q else 1.0
        for c in range(CHUNKS - 1):
            block = [jnp.zeros((OWN * (c + 1), ROWS), F32)]
            block += [sums[k][:, ROWS * c : ROWS * c + ROWS] * sign for k in range(c + 1, CHUNKS)]
            flipped = jnp.concatenate(block, 0).T.astype(BF16)
            for r in range(N_TM):
                mirror_ref[r, q, OWN * c : OWN * c + OWN, :] = flipped[OWN * r : OWN * r + OWN]


def mirror(terms):
    return pl.pallas_call(
        mirror_kernel,
        in_specs=[VMEM] * CHUNKS,
        out_specs=(VMEM, VMEM),
        out_shape=(
            jax.ShapeDtypeStruct((2, OWN * CHUNKS, ROWS * CHUNKS), F32),
            jax.ShapeDtypeStruct((N_TM, 2, OWN * (CHUNKS - 1), OWN * CHUNKS), BF16),
        ),
        compiler_params=params(8),
        cost_estimate=cost(1 << 28, 1 << 22),
        name="mirror",
    )(*terms)


def place_kernel(sums_ref, mirror_ref, wide_ref, narrow_ref, out_ref):
    wide = wide_ref[...]
    narrow = narrow_ref[...]
    lanes = OWN * CHUNKS
    spare = jnp.zeros((OWN, lanes), BF16)
    for q in (0, 1):
        for u in (0, 1):
            part = jnp.concatenate(
                [sums_ref[q, :, ROWS * c + 128 * u : ROWS * c + 128 * u + 128] for c in range(CHUNKS)], 1
            )
            high = part.astype(BF16)
            low = (part - high.astype(F32)).astype(BF16)
            placed = dot_nn(high, wide) + dot_nn(low, wide)
            for w in range(4):
                r = 4 * u + w
                other = jnp.concatenate([mirror_ref[r, q], spare], 0)
                tile = placed[:, 128 * w : 128 * w + 128] + dot_nn(other, narrow)
                for c in range(CHUNKS):
                    for s in range(4):
                        out_ref[q, 32 * s + IC * c : 32 * s + IC * c + IC, 128 * r : 128 * r + 128] = tile[
                            OWN * c + IC * s : OWN * c + IC * s + IC
                        ]


def place(sums, mirrored, wide, narrow):
    return pl.pallas_call(
        place_kernel,
        in_specs=[VMEM] * 4,
        out_specs=VMEM,
        out_shape=jax.ShapeDtypeStruct((2, OWN * CHUNKS, 1024), F32),
        compiler_params=params(8),
        cost_estimate=cost(1 << 28, 1 << 22),
        name="place",
    )(sums, mirrored, wide, narrow)


def beam_kernel(*refs):
    chunks, weight_ref, out_ref = refs[:CHUNKS], refs[CHUNKS], refs[-1]
    total = None
    for p in (0, 1):
        for c in range(CHUNKS):
            column = (p * CHUNKS + c) * ROWS
            term = dot_nn(weight_ref[:, column : column + ROWS], chunks[c][:, HALF * p : HALF * p + HALF])
            total = term if total is None else total + term
    out_ref[...] = total.T.astype(BF16)


def beam_sum(chunks, weights):
    return pl.pallas_call(
        beam_kernel,
        in_specs=[VMEM] * (CHUNKS + 1),
        out_specs=VMEM,
        out_shape=jax.ShapeDtypeStruct((HALF, HALF), BF16),
        compiler_params=params(10),
        cost_estimate=cost(1 << 29, 1 << 22),
        name="beams",
    )(*chunks, weights)


def exchange(array, axes):
    return lax.all_to_all(array, axes, 0, 0, tiled=True)


def to_everyone(array, axes, count):
    return exchange(jnp.broadcast_to(array[None], (count, *array.shape)), axes)


def body(voltages, beam_weights):
    tables = tuple(
        jnp.asarray(t, BF16 if k in (0, 3) else F32) for k, t in enumerate(dft_tables())
    )
    signal = voltages.reshape(2, N_STAT, SPECTRA, 32, 128).transpose(0, 1, 3, 2, 4)
    signal = signal.reshape(2, N_STAT, 128, 128)

    own_piece = lax.axis_index(TM)
    pieces = beam_weights.reshape(N_TM, IC, 256)
    piece = lax.dynamic_index_in_dim(pieces, own_piece, 0, keepdims=False)
    gathered = to_everyone(to_everyone(piece, STAT, N_STAT), TM, N_TM)
    flat = gathered.reshape(2, CHUNKS * ROWS, 256).transpose(0, 2, 1)
    weights = jnp.concatenate(
        [jnp.concatenate([flat[0], -flat[1]], 1), jnp.concatenate([flat[1], flat[0]], 1)], 0
    )

    chunks = []
    terms = []
    for c in range(CHUNKS):
        ready = dft_chunk(signal, tables, c)
        chunks.append(exchange(ready, STAT).reshape(ROWS, 1024))
        terms.append(exchange(gram(chunks), TM))
    terms = [t.astype(F32).sum(0) for t in terms[:-1]] + terms[-1:]
    beams = beam_sum(chunks, weights).reshape(NF // N_STAT, SPECTRA, 2, 256)
    sums, mirrored = mirror(terms)
    mirrored = exchange(mirrored, TM)
    wide = jnp.asarray(natural_order(4), BF16)
    narrow = jnp.asarray(natural_order(1), BF16)
    rows = place(sums, mirrored, wide, narrow)
    return beams, rows.transpose(1, 0, 2)[:, None]


def solution(mesh):
    finer = Mesh(
        mesh.devices.reshape(2, 8, 2, 4, 2), ("stat_0", "stat_1", "stat_2", "tm_0", "tm_1")
    )
    return jax.shard_map(
        body,
        mesh=finer,
        in_specs=(P(None, STAT, TM, None), P(None, STAT, None)),
        out_specs=(P(STAT, TM, None, None), P(TM, STAT, None, None)),
        check_vma=False,
    )
```

```python
import math

import jax
import jax.numpy as jnp
import numpy as np
from jax import lax
from jax.experimental import pallas as pl
from jax.experimental.pallas import tpu as pltpu
from jax.sharding import Mesh
from jax.sharding import PartitionSpec as P


STAT = ("stat_0", "stat_1", "stat_2")
CHIP = ("stat_0", "stat_1")
TM = ("tm_0", "tm_1")
NF = 4096
CHIPS = 16
N_TM = 8
SPECTRA = 4
FIRST, SECOND = 24, 8
SIDE_A, SIDE_B = CHIPS * FIRST, CHIPS * SECOND
OWN_A, OWN_B = SIDE_A // N_TM, SIDE_B // N_TM
COLS_A, COLS_B = 2 * SIDE_A, 2 * SIDE_B
HALF = 512
BF16 = jnp.bfloat16
F32 = jnp.float32
VMEM = pl.BlockSpec(memory_space=pltpu.VMEM)
SMEM = pl.BlockSpec(memory_space=pltpu.SMEM)
ANY = pl.BlockSpec(memory_space=pl.ANY)


def rotation(angle):
    cosine, sine = np.cos(angle), np.sin(angle)
    return np.block([[cosine, sine], [-sine, cosine]])


def dft_tables():
    outer = np.arange(32)
    angle = 2.0 * np.pi * np.outer(outer, outer) / 32
    eye = np.eye(SPECTRA)
    spread = lambda m: np.einsum("wc,st->wsct", m, eye).reshape(128, 128)
    cosine, sine = spread(np.cos(angle)), spread(np.sin(angle))
    left = np.block([[cosine, sine], [-sine, cosine]])
    w0 = np.repeat(np.arange(32), SPECTRA)
    twist = 2.0 * np.pi * np.outer(w0, np.arange(128)) / NF
    inner = 2.0 * np.pi * np.outer(np.arange(128), np.arange(128)) / 128
    right = rotation(inner) / math.sqrt(NF)
    right = right.reshape(2, 32, 4, 256).transpose(1, 0, 2, 3).reshape(256, 256)
    return (
        left.astype(np.float32),
        np.cos(twist).astype(np.float32),
        np.sin(twist).astype(np.float32),
        right.astype(np.float32),
    )


def natural_columns():
    core, chip, item = np.meshgrid(np.arange(2), np.arange(CHIPS), np.arange(32), indexing="ij")
    place = 32 * (2 * chip + core) + item
    return np.concatenate([place[:, :, :FIRST].reshape(-1), place[:, :, FIRST:].reshape(-1)])


def params(mib):
    return pltpu.CompilerParams(vmem_limit_bytes=mib * 1024 * 1024)


def cost(macs, moved):
    return pl.CostEstimate(flops=2 * macs, bytes_accessed=moved, transcendentals=0)


def dot_nn(a, b):
    return lax.dot_general(a, b, (((1,), (0,)), ((), ())), preferred_element_type=F32)


def dot_nt(a, b):
    return lax.dot_general(a, b, (((1,), (1,)), ((), ())), preferred_element_type=F32)


def dft_kernel(place_ref, x_ref, left_ref, cos_ref, sin_ref, right_ref, out_ref, stage):
    count = x_ref.shape[1]
    core = place_ref[0]
    left = left_ref[...]
    right = right_ref[...]
    cosine = cos_ref[...]
    sine = sin_ref[...]
    for pair in range(count // 2):
        signal = [jnp.concatenate([x_ref[0, 2 * pair + k], x_ref[1, 2 * pair + k]], 0) for k in (0, 1)]
        first = dot_nn(left, jnp.concatenate(signal, 1))
        turned = []
        for k in (0, 1):
            re = first[:128, 128 * k : 128 * k + 128]
            im = first[128:, 128 * k : 128 * k + 128]
            turned.append(
                jnp.concatenate(
                    [(re * cosine + im * sine).astype(BF16), (im * cosine - re * sine).astype(BF16)], 1
                )
            )
        final = dot_nt(right, jnp.concatenate(turned, 0))
        for k in (0, 1):
            stage[pl.ds(2 * pair + k, 256, stride=count), :] = final[:, 128 * k : 128 * k + 128]
    for chip in range(CHIPS):
        for side in (0, 1):
            for t in range(8):
                row = ((2 * chip + side) * 8 + t) * count
                out_ref[chip, side ^ core, :, 128 * t : 128 * t + 128] = stage[row : row + count, :].astype(BF16)


def dft_part(place, signal, tables, count, index):
    full = lambda a: pl.BlockSpec(a.shape, lambda i: (0,) * a.ndim)
    return pl.pallas_call(
        dft_kernel,
        grid=(1,),
        in_specs=[SMEM, pl.BlockSpec((2, count, 128, 128), lambda i: (0, index, 0, 0))]
        + [full(t) for t in tables],
        out_specs=pl.BlockSpec((CHIPS, 2, count, 1024), lambda i: (0, 0, 0, 0)),
        out_shape=jax.ShapeDtypeStruct((CHIPS, 2, count, 1024), BF16),
        scratch_shapes=[pltpu.VMEM((256 * count, 128), F32)],
        compiler_params=params(16),
        cost_estimate=cost(count << 25, count << 17),
    )(place, signal, *tables)


def put_sides(core, kept, swapped, out_ref):
    side = kept.shape[0]
    out_ref[pl.ds(pl.multiple_of(core * side, side), side), :] = kept
    out_ref[pl.ds(pl.multiple_of((1 - core) * side, side), side), :] = swapped


def product(rows, cols):
    scale = 1.0 / NF
    real = dot_nt(rows, cols) * scale
    imag = (dot_nt(rows[:, HALF:], cols[:, :HALF]) - dot_nt(rows[:, :HALF], cols[:, HALF:])) * scale
    return real, imag


def gram_first_kernel(place_ref, kept_ref, swapped_ref, spec_ref, *rest):
    out_refs, full = rest[:N_TM], rest[N_TM]
    put_sides(place_ref[0], kept_ref[...], swapped_ref[...], spec_ref)
    own = place_ref[1]
    for a in (0, 1):
        width = SIDE_A * (a + 1)
        start = SIDE_A * a
        values = product(spec_ref[start : start + SIDE_A, :], spec_ref[:width, :])
        for q in (0, 1):
            full[q, :, start : start + width] = values[q].astype(BF16)
    for k in range(N_TM):
        row = pl.multiple_of((own ^ k) * OWN_A, OWN_A)
        for q in (0, 1):
            out_refs[k][q] = full[q, pl.ds(row, OWN_A), :]


def gram_first(place, kept, swapped):
    width = 3 * SIDE_A
    return pl.pallas_call(
        gram_first_kernel,
        in_specs=[SMEM, VMEM, VMEM],
        out_specs=(VMEM,) * (N_TM + 1),
        out_shape=(jax.ShapeDtypeStruct((COLS_A, 1024), BF16),)
        + (jax.ShapeDtypeStruct((2, OWN_A, width), BF16),) * N_TM,
        scratch_shapes=[pltpu.VMEM((2, SIDE_A, width), BF16)],
        compiler_params=params(16),
        cost_estimate=cost(1 << 30, 6 << 20),
        name="gram_first",
    )(place, kept, swapped)


def gram_second_kernel(place_ref, kept_ref, swapped_ref, first_ref, spec_ref, out_ref):
    put_sides(place_ref[0], kept_ref[...], swapped_ref[...], spec_ref)
    mine = spec_ref[...]
    against_first = product(mine, first_ref[...])
    against_second = product(mine, mine)
    for q in (0, 1):
        flipped = against_first[q].T
        flipped = (-flipped if q else flipped).astype(BF16)
        blocks = [against_first[q][:, COLS_B * j : COLS_B * j + COLS_B].astype(BF16) for j in range(3)]
        blocks.append(against_second[q].astype(BF16))
        for r in range(N_TM):
            for j in range(4):
                for a in (0, 1):
                    row = 2 * OWN_B * j + OWN_B * a
                    src = SIDE_B * a + OWN_B * r
                    out_ref[r, q, row : row + OWN_B, :] = blocks[j][src : src + OWN_B]
            for a in (0, 1):
                row = 8 * OWN_B + OWN_A * a
                src = SIDE_A * a + OWN_A * r
                out_ref[r, q, row : row + OWN_A, :] = flipped[src : src + OWN_A]


def gram_second(place, kept, swapped, first):
    rows = 8 * OWN_B + 2 * OWN_A
    return pl.pallas_call(
        gram_second_kernel,
        in_specs=[SMEM, VMEM, VMEM, VMEM],
        out_specs=(VMEM, VMEM),
        out_shape=(
            jax.ShapeDtypeStruct((COLS_B, 1024), BF16),
            jax.ShapeDtypeStruct((N_TM, 2, rows, COLS_B), BF16),
        ),
        compiler_params=params(20),
        cost_estimate=cost(1 << 29, 6 << 20),
        name="gram_second",
    )(place, kept, swapped, first)


def mirror_kernel(place_ref, *refs):
    terms, sums_ref, mirror_refs, flip = refs[:N_TM], refs[N_TM + 1], refs[N_TM + 2 : -1], refs[-1]
    own = place_ref[1]
    for q in (0, 1):
        total = terms[0][q].astype(F32)
        for k in range(1, N_TM):
            total = total + terms[k][q].astype(F32)
        sums_ref[q, :OWN_A, :SIDE_A] = total[:, :SIDE_A]
        sums_ref[q, :OWN_A, SIDE_A:] = jnp.zeros((OWN_A, SIDE_A), F32)
        sums_ref[q, OWN_A:, :] = total[:, SIDE_A:]
        block = total[:, SIDE_A : 2 * SIDE_A] * (-1.0 if q else 1.0)
        block = jnp.concatenate([block, jnp.zeros((128 - OWN_A, SIDE_A), F32)], 0)
        flip[q] = block.T
        for k in range(1, N_TM):
            row = pl.multiple_of((own ^ k) * OWN_A, OWN_A)
            mirror_refs[k][q] = flip[q, pl.ds(row, OWN_A), :].astype(BF16)
        row = pl.multiple_of(own * OWN_A, OWN_A)
        mirror_refs[0][q] = flip[q, pl.ds(row, OWN_A), :].astype(BF16)


def mirror(place, terms, after):
    return pl.pallas_call(
        mirror_kernel,
        in_specs=[SMEM] + [VMEM] * N_TM + [ANY],
        out_specs=(VMEM,) * (N_TM + 1),
        out_shape=(jax.ShapeDtypeStruct((2, 2 * OWN_A, COLS_A), F32),)
        + (jax.ShapeDtypeStruct((2, OWN_A, 128), BF16),) * N_TM,
        scratch_shapes=[pltpu.VMEM((2, SIDE_A, 128), F32)],
        compiler_params=params(8),
        cost_estimate=cost(1 << 27, 1 << 21),
        name="mirror",
    )(place, *terms, after)


def spread_kernel(place_ref, sums_ref, order_ref, narrow_ref, *refs):
    mirrors, out_ref = refs[:N_TM], refs[-1]
    own = place_ref[1]
    order = order_ref[:COLS_A, :]
    narrow = narrow_ref[...]
    for q in (0, 1):
        total = sums_ref[q]
        high = total.astype(BF16)
        low = (total - high.astype(F32)).astype(BF16)
        out_ref[q] = dot_nn(high, order) + dot_nn(low, order)
        for k in range(N_TM):
            col = pl.multiple_of((own ^ k) * 128, 128)
            out_ref[q, :OWN_A, pl.ds(col, 128)] += dot_nn(mirrors[k][q], narrow)


def spread_first(place, sums, order, narrow, mirrors):
    return pl.pallas_call(
        spread_kernel,
        in_specs=[SMEM] + [VMEM] * (N_TM + 3),
        out_specs=VMEM,
        out_shape=jax.ShapeDtypeStruct((2, 2 * OWN_A, 1024), F32),
        compiler_params=params(8),
        cost_estimate=cost(1 << 28, 1 << 22),
        name="spread_first",
    )(place, sums, order, narrow, *mirrors)


def finish_kernel(terms_ref, base_ref, order_ref, out_ref):
    order = order_ref[...]
    for q in (0, 1):
        total = terms_ref[0, q].astype(F32)
        for t in range(1, N_TM):
            total = total + terms_ref[t, q].astype(F32)
        rows_b = 2 * OWN_B
        last = jnp.concatenate([total[rows_b * j : rows_b * j + rows_b] for j in range(4)], 1)
        extra = total[4 * rows_b :]

        def placed(value, table):
            high = value.astype(BF16)
            low = (value - high.astype(F32)).astype(BF16)
            return dot_nn(high, table) + dot_nn(low, table)

        lower = placed(last, order)
        upper = base_ref[q] + placed(extra, order[COLS_A:])
        for a in (0, 1):
            for chip in (0, 1):
                row = 64 * chip + 32 * a
                src = OWN_A * a + FIRST * chip
                out_ref[q, row : row + FIRST, :] = upper[src : src + FIRST]
                src = OWN_B * a + SECOND * chip
                out_ref[q, row + FIRST : row + 32, :] = lower[src : src + SECOND]


def finish(terms, base, order):
    return pl.pallas_call(
        finish_kernel,
        in_specs=[VMEM] * 3,
        out_specs=VMEM,
        out_shape=jax.ShapeDtypeStruct((2, 128, 1024), F32),
        compiler_params=params(8),
        cost_estimate=cost(1 << 28, 1 << 22),
        name="finish",
    )(terms, base, order)


def weight_kernel(place_ref, *refs):
    blocks, out_ref, rows_a, rows_b = refs[:N_TM], refs[N_TM], refs[-2], refs[-1]
    core, own, far, z = place_ref[0], place_ref[1], place_ref[2], place_ref[3]
    for k in range(N_TM):
        source = (z - (own ^ k)) & 7
        for dx in (0, 1):
            for dc in (0, 1):
                chip = (far ^ dx) * 8 + source
                side = core ^ dc
                row_a = pl.multiple_of(side * SIDE_A + chip * FIRST, 8)
                row_b = pl.multiple_of(side * SIDE_B + chip * SECOND, 8)
                for p in (0, 1):
                    block = blocks[k][dx, dc, p].astype(F32)
                    rows_a[p, pl.ds(row_a, FIRST), :] = block[:FIRST]
                    rows_b[p, pl.ds(row_b, SECOND), :] = block[FIRST:]
    for p in (0, 1):
        flipped = jnp.concatenate([rows_a[p].T, rows_b[p].T], 1)
        straight = flipped.astype(BF16)
        out_ref[:256, 1024 * p : 1024 * p + 1024] = (-flipped).astype(BF16) if p else straight
        out_ref[256:, 1024 * (1 - p) : 1024 * (1 - p) + 1024] = straight


def weight_stack(place, blocks):
    return pl.pallas_call(
        weight_kernel,
        in_specs=[SMEM] + [VMEM] * N_TM,
        out_specs=VMEM,
        out_shape=jax.ShapeDtypeStruct((HALF, 2048), BF16),
        scratch_shapes=[pltpu.VMEM((2, COLS_A, 256), F32), pltpu.VMEM((2, COLS_B, 256), F32)],
        compiler_params=params(12),
        cost_estimate=cost(1 << 27, 1 << 22),
        name="weights",
    )(place, *blocks)


def beam_kernel(first_ref, second_ref, weight_ref, after_ref, out_ref):
    total = None
    for p in (0, 1):
        lanes = slice(HALF * p, HALF * p + HALF)
        middle = 1024 * p + COLS_A
        term = dot_nn(weight_ref[:, 1024 * p : middle], first_ref[:, lanes])
        term = term + dot_nn(weight_ref[:, middle : middle + COLS_B], second_ref[:, lanes])
        total = term if total is None else total + term
    out_ref[...] = total.T.astype(BF16)


def beam_sum(first, second, weights, after):
    return pl.pallas_call(
        beam_kernel,
        in_specs=[VMEM] * 3 + [ANY],
        out_specs=VMEM,
        out_shape=jax.ShapeDtypeStruct((HALF, HALF), BF16),
        compiler_params=params(12),
        cost_estimate=cost(1 << 29, 1 << 22),
        name="beams",
    )(first, second, weights, after)


def swap(array, axis):
    return lax.ppermute(array, axis, [(0, 1), (1, 0)])


def with_partners(array):
    pairs = lambda k: [(i, i ^ k) for i in range(N_TM)]
    return [array] + [lax.ppermute(array, TM, pairs(k)) for k in range(1, N_TM)]


def to_partners(arrays):
    pairs = lambda k: [(i, i ^ k) for i in range(N_TM)]
    return [arrays[0]] + [lax.ppermute(arrays[k], TM, pairs(k)) for k in range(1, N_TM)]


def turn(ready, count):
    arrived = lax.all_to_all(ready, CHIP, 0, 0, tiled=True)
    kept = arrived[:, 0].reshape(CHIPS * count, 1024)
    other = arrived[:, 1].reshape(CHIPS * count, 1024)
    swapped = swap(other, "stat_2")
    return kept, swapped


def behind(value, other):
    return lax.optimization_barrier((value, other))[0]


def step(voltages, beam_weights):
    tables = tuple(jnp.asarray(t, BF16 if k in (0, 3) else F32) for k, t in enumerate(dft_tables()))
    signal = voltages.reshape(2, 32, SPECTRA, 32, 128).transpose(0, 1, 3, 2, 4)
    signal = signal.reshape(2, 32, 128, 128)
    where = ("stat_2", TM, "stat_0", "stat_1")
    place = jnp.stack([lax.axis_index(a) for a in where]).astype(jnp.int32)

    ready_a = dft_part(place, signal, tables, FIRST, 0)
    ready_b = dft_part(place, signal, tables, SECOND, FIRST // SECOND)

    block = behind(beam_weights, ready_b)
    ring = [(z * N_TM + t, (z + t) % 8 * N_TM + t) for z in range(8) for t in range(N_TM)]
    block = lax.ppermute(block, ("stat_1", *TM), ring)
    block = jnp.stack([block, swap(block, "stat_2")])
    block = jnp.stack([block, swap(block, "stat_0")])
    blocks_k = with_partners(block)
    weights = weight_stack(place, blocks_k)
    columns = behind(jnp.asarray(natural_columns(), jnp.int32), ready_b)
    order = (columns[:, None] == jnp.arange(1024, dtype=jnp.int32)[None, :]).astype(BF16)
    item = np.arange(128)
    target = np.where(item < OWN_A, 64 * (item // FIRST) + 32 + item % FIRST, -1)
    narrow = jnp.asarray((target[:, None] == item[None, :]), BF16)

    kept_a, swapped_a = turn(ready_a, FIRST)
    kept_b, swapped_b = turn(ready_b, SECOND)
    first, *terms = gram_first(place, kept_a, swapped_a)
    arrived = to_partners(terms)
    second, blocks = gram_second(place, kept_b, swapped_b, first)
    last = lax.all_to_all(blocks, TM, 0, 0, tiled=True)

    sums, *mirrors = mirror(place, arrived, blocks)
    mirrors = to_partners(mirrors)
    base = spread_first(place, sums, order, narrow, mirrors)
    beams = beam_sum(first, second, weights, blocks)
    beams = beams.reshape(NF // 32, SPECTRA, 2, 256)
    rows = finish(last, base, order)
    return beams, rows.transpose(1, 0, 2)[:, None]


def solution(mesh):
    finer = Mesh(
        mesh.devices.reshape(2, 8, 2, 4, 2), ("stat_0", "stat_1", "stat_2", "tm_0", "tm_1")
    )
    return jax.shard_map(
        step,
        mesh=finer,
        in_specs=(P(None, STAT, TM, None), P(None, STAT, None)),
        out_specs=(P(STAT, TM, None, None), P(TM, STAT, None, None)),
        check_vma=False,
    )
```

```python
import math

import jax
import jax.numpy as jnp
import numpy as np
from jax import lax
from jax.experimental import pallas as pl
from jax.experimental.pallas import tpu as pltpu
from jax.sharding import Mesh
from jax.sharding import PartitionSpec as P


STAT = ("stat_0", "stat_1", "stat_2")
CHIP = ("stat_0", "stat_1")
TM = ("tm_0", "tm_1")
NF = 4096
CHIPS = 16
N_TM = 8
SPECTRA = 4
FIRST, SECOND = 24, 8
SIDE_A, SIDE_B = CHIPS * FIRST, CHIPS * SECOND
OWN_A, OWN_B = SIDE_A // N_TM, SIDE_B // N_TM
COLS_A, COLS_B = 2 * SIDE_A, 2 * SIDE_B
HALF = 512
BF16 = jnp.bfloat16
F32 = jnp.float32
VMEM = pl.BlockSpec(memory_space=pltpu.VMEM)
SMEM = pl.BlockSpec(memory_space=pltpu.SMEM)
ANY = pl.BlockSpec(memory_space=pl.ANY)
HBM = pl.BlockSpec(memory_space=pltpu.HBM)


def rotation(angle):
    cosine, sine = np.cos(angle), np.sin(angle)
    return np.block([[cosine, sine], [-sine, cosine]])


def dft_tables():
    outer = np.arange(32)
    angle = 2.0 * np.pi * np.outer(outer, outer) / 32
    eye = np.eye(SPECTRA)
    spread = lambda m: np.einsum("wc,st->wsct", m, eye).reshape(128, 128)
    cosine, sine = spread(np.cos(angle)), spread(np.sin(angle))
    left = np.block([[cosine, sine], [-sine, cosine]])
    w0 = np.repeat(np.arange(32), SPECTRA)
    twist = 2.0 * np.pi * np.outer(w0, np.arange(128)) / NF
    inner = 2.0 * np.pi * np.outer(np.arange(128), np.arange(128)) / 128
    right = rotation(inner) / math.sqrt(NF)
    right = right.reshape(2, 32, 4, 256).transpose(1, 0, 2, 3).reshape(256, 256)
    return (
        left.astype(np.float32),
        np.cos(twist).astype(np.float32),
        np.sin(twist).astype(np.float32),
        right.astype(np.float32),
    )


def natural_columns(core):
    def of(core):
        rel, chip, item = np.meshgrid(np.arange(2), np.arange(CHIPS), np.arange(32), indexing="ij")
        place = 32 * (2 * chip + (rel ^ core)) + item
        late = place[:, :, FIRST:].transpose(1, 0, 2)
        return np.concatenate([place[:, :, :FIRST].reshape(-1), late.reshape(-1)]).astype(np.int32)

    return jnp.where(core == 0, jnp.asarray(of(0)), jnp.asarray(of(1)))


def params(mib):
    return pltpu.CompilerParams(vmem_limit_bytes=mib * 1024 * 1024)


def cost(macs, moved):
    return pl.CostEstimate(flops=2 * macs, bytes_accessed=moved, transcendentals=0)


def dot_nn(a, b):
    return lax.dot_general(a, b, (((1,), (0,)), ((), ())), preferred_element_type=F32)


def dot_nt(a, b):
    return lax.dot_general(a, b, (((1,), (1,)), ((), ())), preferred_element_type=F32)


def dft_kernel(place_ref, x_hbm, left_hbm, turn_hbm, right_hbm, *refs):
    outs, (x_ref, left_ref, turn_ref, right_ref, stage, sems, pack, out_sems) = refs[:-8], refs[-8:]
    count = x_ref.shape[1]
    start = 0 if count == FIRST else FIRST
    loads = [
        pltpu.make_async_copy(left_hbm, left_ref, sems.at[0]),
        pltpu.make_async_copy(turn_hbm, turn_ref, sems.at[1]),
        pltpu.make_async_copy(right_hbm, right_ref, sems.at[2]),
    ]
    groups = count // 8
    for g in range(groups):
        loads.append(
            pltpu.make_async_copy(
                x_hbm.at[:, start + 8 * g : start + 8 * g + 8], x_ref.at[:, 8 * g : 8 * g + 8], sems.at[3 + g]
            )
        )
    for load in [loads[0], loads[3], *loads[1:3], *loads[4:]]:
        load.start()
    for load in loads[:3]:
        load.wait()
    core = place_ref[0]
    left = left_ref[...]
    right = right_ref[...]
    cosine = turn_ref[0]
    sine = turn_ref[1]
    for pair in range(count // 2):
        if pair % 4 == 0:
            loads[3 + pair // 4].wait()
        signal = [jnp.concatenate([x_ref[0, 2 * pair + k], x_ref[1, 2 * pair + k]], 0) for k in (0, 1)]
        first = dot_nn(left, jnp.concatenate(signal, 1))
        turned = []
        for k in (0, 1):
            re = first[:128, 128 * k : 128 * k + 128]
            im = first[128:, 128 * k : 128 * k + 128]
            turned.append(
                jnp.concatenate(
                    [(re * cosine + im * sine).astype(BF16), (im * cosine - re * sine).astype(BF16)], 1
                )
            )
        final = dot_nt(right, jnp.concatenate(turned, 0))
        for k in (0, 1):
            stage[pl.ds(2 * pair + k, 256, stride=count), :] = final[:, 128 * k : 128 * k + 128]
    stores = []
    for chip in range(CHIPS):
        for rel in (0, 1):
            for t in range(8):
                row = pl.multiple_of(((2 * chip + (rel ^ core)) * 8 + t) * count, 8)
                value = stage[pl.ds(row, count), :].astype(BF16)
                if len(outs) == 1:
                    pack[chip, rel, :, 128 * t : 128 * t + 128] = value
                else:
                    outs[rel][chip, :, 128 * t : 128 * t + 128] = value
        if len(outs) == 1:
            stores.append(pltpu.make_async_copy(pack.at[chip], outs[0].at[chip], out_sems.at[chip]))
            stores[chip].start()
    for store in stores:
        store.wait()


def dft_part(place, signal, tables, count):
    full = pltpu.HBM((CHIPS, 2, count, 1024), BF16)
    half = jax.ShapeDtypeStruct((CHIPS, count, 1024), BF16)
    shapes = (full,) if count == FIRST else (half, half)
    return pl.pallas_call(
        dft_kernel,
        in_specs=[SMEM] + [HBM] * 4,
        out_specs=(HBM,) if count == FIRST else (VMEM, VMEM),
        out_shape=shapes,
        scratch_shapes=[
            pltpu.VMEM((2, count, 128, 128), BF16),
            pltpu.VMEM((256, 256), BF16),
            pltpu.VMEM((2, 128, 128), F32),
            pltpu.VMEM((256, 256), BF16),
            pltpu.VMEM((256 * count, 128), F32),
            pltpu.SemaphoreType.DMA((3 + count // 8,)),
            pltpu.VMEM((CHIPS if count == FIRST else 1, 2, count, 1024), BF16),
            pltpu.SemaphoreType.DMA((CHIPS,)),
        ],
        compiler_params=params(60 if count == FIRST else 12),
        cost_estimate=cost(count << 25, count << 17),
    )(place, signal, *tables)


def product(rows, cols):
    scale = 1.0 / NF
    real = dot_nt(rows, cols) * scale
    imag = (dot_nt(rows[:, HALF:], cols[:, :HALF]) - dot_nt(rows[:, :HALF], cols[:, HALF:])) * scale
    return real, imag


def gram_first_kernel(place_ref, kept_ref, swapped_ref, *rest):
    out_refs, full = rest[:N_TM], rest[N_TM]
    own = place_ref[1]
    sides = (kept_ref, swapped_ref)
    for a in (0, 1):
        for b in (0, 1):
            values = product(sides[a][...], sides[b][...])
            for q in (0, 1):
                full[q, a, :, SIDE_A * b : SIDE_A * b + SIDE_A] = values[q].astype(BF16)
    for k in range(N_TM):
        row = pl.multiple_of((own ^ k) * OWN_A, OWN_A)
        for q in (0, 1):
            for a in (0, 1):
                out_refs[k][q, OWN_A * a : OWN_A * a + OWN_A] = full[q, a, pl.ds(row, OWN_A), :]


def gram_first(place, kept, swapped):
    return pl.pallas_call(
        gram_first_kernel,
        in_specs=[SMEM, VMEM, VMEM],
        out_specs=(VMEM,) * N_TM,
        out_shape=(jax.ShapeDtypeStruct((2, 2 * OWN_A, COLS_A), BF16),) * N_TM,
        scratch_shapes=[pltpu.VMEM((2, 2, SIDE_A, COLS_A), BF16)],
        compiler_params=params(10),
        cost_estimate=cost(1 << 30, 6 << 20),
        name="gram_first",
    )(place, kept, swapped)


def gram_second_kernel(mine_ref, kept_ref, swapped_ref, out_hbm, out_ref, sems):
    mine = mine_ref[...]
    sides = [product(mine, kept_ref[...]), product(mine, swapped_ref[...])]
    second = product(mine, mine)
    copies = []
    for q in (0, 1):
        first = jnp.concatenate([sides[0][q], sides[1][q]], 1)
        flipped = first.T
        flipped = (-flipped if q else flipped).astype(BF16)
        blocks = [first[:, COLS_B * j : COLS_B * j + COLS_B].astype(BF16) for j in range(3)]
        blocks.append(second[q].astype(BF16))
        rows = 2 * OWN_B
        for r in range(N_TM):
            for j in range(4):
                out_ref[r, q, rows * j : rows * j + rows, :] = blocks[j][rows * r : rows * r + rows]
            for a in (0, 1):
                row = 4 * rows + OWN_A * a
                src = SIDE_A * a + OWN_A * r
                out_ref[r, q, row : row + OWN_A, :] = flipped[src : src + OWN_A]
        copies.append(pltpu.make_async_copy(out_ref.at[:, q], out_hbm.at[:, q], sems.at[q]))
        copies[q].start()
    for copy in copies:
        copy.wait()


def gram_second(mine, kept, swapped):
    rows = 8 * OWN_B + 2 * OWN_A
    return pl.pallas_call(
        gram_second_kernel,
        in_specs=[VMEM, VMEM, VMEM],
        out_specs=HBM,
        out_shape=pltpu.HBM((N_TM, 2, rows, COLS_B), BF16),
        scratch_shapes=[
            pltpu.VMEM((N_TM, 2, rows, COLS_B), BF16),
            pltpu.SemaphoreType.DMA((2,)),
        ],
        compiler_params=params(10),
        cost_estimate=cost(1 << 29, 6 << 20),
        name="gram_second",
    )(mine, kept, swapped)


def placed(values, table):
    parts = []
    for value in values:
        high = value.astype(BF16)
        parts += [high, (value - high.astype(F32)).astype(BF16)]
    result = dot_nn(jnp.concatenate(parts, 0), table)
    size = values[0].shape[0]
    return [result[2 * k * size : (2 * k + 1) * size] + result[(2 * k + 1) * size : (2 * k + 2) * size] for k in range(len(values))]


def spread_kernel(*refs):
    terms, order_ref, out_ref = refs[:N_TM], refs[N_TM], refs[-1]
    totals = []
    for q in (0, 1):
        total = terms[0][q].astype(F32)
        for k in range(1, N_TM):
            total = total + terms[k][q].astype(F32)
        totals.append(total)
    spread = placed(totals, order_ref[:COLS_A, :])
    for q in (0, 1):
        out_ref[q] = spread[q]


def spread_first(terms, order):
    return pl.pallas_call(
        spread_kernel,
        in_specs=[VMEM] * (N_TM + 1),
        out_specs=VMEM,
        out_shape=jax.ShapeDtypeStruct((2, 2 * OWN_A, 1024), F32),
        compiler_params=params(8),
        cost_estimate=cost(1 << 28, 1 << 22),
        name="spread_first",
    )(*terms, order)


def finish_kernel(place_ref, terms_ref, base_ref, order_ref, out_ref):
    core = place_ref[0]
    rows = 2 * OWN_B
    last, extra = [], []
    for q in (0, 1):
        total = terms_ref[0, q].astype(F32)
        for t in range(1, N_TM):
            total = total + terms_ref[t, q].astype(F32)
        last.append(jnp.concatenate([total[rows * j : rows * j + rows] for j in range(4)], 1))
        extra.append(total[4 * rows :])
    lower = placed(last, order_ref[...])
    upper = placed(extra, order_ref[COLS_A:, :])
    for q in (0, 1):
        top = base_ref[q] + upper[q]
        for rel in (0, 1):
            for chip in (0, 1):
                row = pl.multiple_of(64 * chip + 32 * (rel ^ core), 8)
                src = OWN_A * rel + FIRST * chip
                out_ref[q, pl.ds(row, FIRST), :] = top[src : src + FIRST]
                src = 2 * SECOND * chip + SECOND * rel
                out_ref[q, pl.ds(pl.multiple_of(row + FIRST, 8), SECOND), :] = lower[q][src : src + SECOND]


def finish(place, terms, base, order):
    return pl.pallas_call(
        finish_kernel,
        in_specs=[SMEM] + [VMEM] * 3,
        out_specs=VMEM,
        out_shape=jax.ShapeDtypeStruct((2, 128, 1024), F32),
        compiler_params=params(8),
        cost_estimate=cost(1 << 28, 1 << 22),
        name="finish",
    )(place, terms, base, order)


def weight_kernel(place_ref, *refs):
    blocks, out_ref, rows = refs[:N_TM], refs[N_TM], refs[-1]
    own, far, z = place_ref[1], place_ref[2], place_ref[3]
    for k in range(N_TM):
        source = (z - (own ^ k)) & 7
        for dx in (0, 1):
            chip = (far ^ dx) * 8 + source
            for dc in (0, 1):
                early = pl.multiple_of(dc * SIDE_A + chip * FIRST, 8)
                late = pl.multiple_of(COLS_A + chip * 2 * SECOND + dc * SECOND, 8)
                for p in (0, 1):
                    block = blocks[k][dc, dx, p].astype(F32)
                    rows[p, pl.ds(early, FIRST), :] = block[:FIRST]
                    rows[p, pl.ds(late, SECOND), :] = block[FIRST:]
    for p in (0, 1):
        flipped = rows[p].T
        straight = flipped.astype(BF16)
        out_ref[:256, 1024 * p : 1024 * p + 1024] = (-flipped).astype(BF16) if p else straight
        out_ref[256:, 1024 * (1 - p) : 1024 * (1 - p) + 1024] = straight


def weight_stack(place, blocks):
    return pl.pallas_call(
        weight_kernel,
        in_specs=[SMEM] + [VMEM] * N_TM,
        out_specs=VMEM,
        out_shape=jax.ShapeDtypeStruct((HALF, 2048), BF16),
        scratch_shapes=[pltpu.VMEM((2, 1024, 256), F32)],
        compiler_params=params(10),
        cost_estimate=cost(1 << 27, 1 << 22),
        name="weights",
    )(place, *blocks)


def beam_kernel(kept_ref, swapped_ref, second_ref, weight_ref, out_ref):
    total = None
    for p in (0, 1):
        lanes = slice(HALF * p, HALF * p + HALF)
        column = 1024 * p
        for ref in (kept_ref, swapped_ref, second_ref):
            count = ref.shape[0]
            term = dot_nn(weight_ref[:, column : column + count], ref[:, lanes])
            column += count
            total = term if total is None else total + term
    out_ref[...] = total.T.astype(BF16)


def beam_sum(kept, swapped, second, weights):
    return pl.pallas_call(
        beam_kernel,
        in_specs=[VMEM] * 4,
        out_specs=VMEM,
        out_shape=jax.ShapeDtypeStruct((HALF, HALF), BF16),
        compiler_params=params(10),
        cost_estimate=cost(1 << 29, 1 << 22),
        name="beams",
    )(kept, swapped, second, weights)


def swap(array, axis):
    return lax.ppermute(array, axis, [(0, 1), (1, 0)])


def with_partners(array):
    pairs = lambda k: [(i, i ^ k) for i in range(N_TM)]
    return [array] + [lax.ppermute(array, TM, pairs(k)) for k in range(1, N_TM)]


def to_partners(arrays):
    pairs = lambda k: [(i, i ^ k) for i in range(N_TM)]
    return [arrays[0]] + [lax.ppermute(arrays[k], TM, pairs(k)) for k in range(1, N_TM)]


def behind(value, other):
    return lax.optimization_barrier((value, other))[0]


def step(voltages, beam_weights):
    left, cosine, sine, right = dft_tables()
    tables = (jnp.asarray(left, BF16), jnp.asarray(np.stack([cosine, sine])), jnp.asarray(right, BF16))
    signal = voltages.reshape(2, 32, SPECTRA, 32, 128).transpose(0, 1, 3, 2, 4)
    signal = signal.reshape(2, 32, 128, 128)
    where = ("stat_2", TM, "stat_0", "stat_1")
    place = jnp.stack([lax.axis_index(a) for a in where]).astype(jnp.int32)

    spots = [(x, z, t) for x in (0, 1) for z in range(8) for t in range(N_TM)]
    at = lambda x, z, t: (x * 8 + z % 8) * N_TM + t
    rings = [[(at(x, z, t), at(x ^ dx, z + t, t)) for x, z, t in spots] for dx in (0, 1)]
    block = jnp.stack([lax.ppermute(beam_weights, (*CHIP, *TM), ring) for ring in rings])

    (ready_a,) = dft_part(place, signal, tables, FIRST)
    own_b, other_b = dft_part(place, signal, tables, SECOND)
    partner_b = swap(other_b, "stat_2")
    ready_b = jnp.concatenate([own_b, partner_b], 1)

    near = swap(block, "stat_2")
    block = jnp.stack([block, near])
    blocks_k = with_partners(block)
    columns = natural_columns(behind(lax.axis_index("stat_2"), ready_b))
    order = (columns[:, None] == jnp.arange(1024, dtype=jnp.int32)[None, :]).astype(BF16)

    arrived = lax.all_to_all(ready_a, CHIP, 0, 0, tiled=True)
    second = lax.all_to_all(ready_b, CHIP, 0, 0, tiled=True).reshape(COLS_B, 1024)
    kept = arrived[:, 0].reshape(SIDE_A, 1024)
    other = arrived[:, 1].reshape(SIDE_A, 1024)
    swapped = swap(other, "stat_2")
    terms = gram_first(place, kept, swapped)
    terms = to_partners(terms)
    blocks = gram_second(second, kept, swapped)
    last = lax.all_to_all(blocks, TM, 0, 0, tiled=True)

    weights = weight_stack(place, blocks_k)
    beams = beam_sum(kept, swapped, second, weights)
    beams = beams.reshape(NF // 32, SPECTRA, 2, 256)
    base = spread_first(terms, order)
    rows = finish(place, last, base, order)
    return beams, rows.transpose(1, 0, 2)[:, None]


def solution(mesh):
    finer = Mesh(
        mesh.devices.reshape(2, 8, 2, 4, 2), ("stat_0", "stat_1", "stat_2", "tm_0", "tm_1")
    )
    return jax.shard_map(
        step,
        mesh=finer,
        in_specs=(P(None, STAT, TM, None), P(None, STAT, None)),
        out_specs=(P(STAT, TM, None, None), P(TM, STAT, None, None)),
        check_vma=False,
    )
```

```python
import math

import jax
import jax.numpy as jnp
import numpy as np
from jax import lax
from jax.experimental import pallas as pl
from jax.experimental.pallas import tpu as pltpu
from jax.sharding import Mesh
from jax.sharding import PartitionSpec as P


STAT = ("stat_0", "stat_1", "stat_2")
CHIP = ("stat_0", "stat_1")
TM = ("tm_0", "tm_1")
NF = 4096
CHIPS = 16
N_TM = 8
SPECTRA = 4
FIRST, SECOND = 16, 16
SIDE_A, SIDE_B = CHIPS * FIRST, CHIPS * SECOND
OWN_A, OWN_B = SIDE_A // N_TM, SIDE_B // N_TM
COLS_A, COLS_B = 2 * SIDE_A, 2 * SIDE_B
PIECES = COLS_A // COLS_B
HALF = 512
BF16 = jnp.bfloat16
F32 = jnp.float32
VMEM = pl.BlockSpec(memory_space=pltpu.VMEM)
SMEM = pl.BlockSpec(memory_space=pltpu.SMEM)
ANY = pl.BlockSpec(memory_space=pl.ANY)
HBM = pl.BlockSpec(memory_space=pltpu.HBM)


def rotation(angle):
    cosine, sine = np.cos(angle), np.sin(angle)
    return np.block([[cosine, sine], [-sine, cosine]])


def dft_tables():
    outer = np.arange(32)
    angle = 2.0 * np.pi * np.outer(outer, outer) / 32
    eye = np.eye(SPECTRA)
    spread = lambda m: np.einsum("wc,st->wsct", m, eye).reshape(128, 128)
    cosine, sine = spread(np.cos(angle)), spread(np.sin(angle))
    left = np.block([[cosine, sine], [-sine, cosine]])
    w0 = np.repeat(np.arange(32), SPECTRA)
    twist = 2.0 * np.pi * np.outer(w0, np.arange(128)) / NF
    inner = 2.0 * np.pi * np.outer(np.arange(128), np.arange(128)) / 128
    right = rotation(inner) / math.sqrt(NF)
    right = right.reshape(2, 32, 4, 256).transpose(1, 0, 2, 3).reshape(256, 256)
    return (
        left.astype(np.float32),
        np.cos(twist).astype(np.float32),
        np.sin(twist).astype(np.float32),
        right.astype(np.float32),
    )


def natural_columns(core):
    def of(core):
        rel, chip, item = np.meshgrid(np.arange(2), np.arange(CHIPS), np.arange(32), indexing="ij")
        place = 32 * (2 * chip + (rel ^ core)) + item
        late = place[:, :, FIRST:].transpose(1, 0, 2)
        return np.concatenate([place[:, :, :FIRST].reshape(-1), late.reshape(-1)]).astype(np.int32)

    return jnp.where(core == 0, jnp.asarray(of(0)), jnp.asarray(of(1)))


def params(mib):
    return pltpu.CompilerParams(vmem_limit_bytes=mib * 1024 * 1024)


def cost(macs, moved):
    return pl.CostEstimate(flops=2 * macs, bytes_accessed=moved, transcendentals=0)


def dot_nn(a, b):
    return lax.dot_general(a, b, (((1,), (0,)), ((), ())), preferred_element_type=F32)


def dot_nt(a, b):
    return lax.dot_general(a, b, (((1,), (1,)), ((), ())), preferred_element_type=F32)


def dft_kernel(place_ref, x_hbm, left_hbm, turn_hbm, right_hbm, *refs):
    outs, (x_ref, left_ref, turn_ref, right_ref, stage, sems, pack, out_sems) = refs[:-8], refs[-8:]
    count = x_ref.shape[1]
    start = 0 if len(outs) == 1 else FIRST
    loads = [
        pltpu.make_async_copy(left_hbm, left_ref, sems.at[0]),
        pltpu.make_async_copy(turn_hbm, turn_ref, sems.at[1]),
        pltpu.make_async_copy(right_hbm, right_ref, sems.at[2]),
    ]
    groups = count // 8
    for g in range(groups):
        loads.append(
            pltpu.make_async_copy(
                x_hbm.at[:, start + 8 * g : start + 8 * g + 8], x_ref.at[:, 8 * g : 8 * g + 8], sems.at[3 + g]
            )
        )
    for load in [loads[0], loads[3], *loads[1:3], *loads[4:]]:
        load.start()
    for load in loads[:3]:
        load.wait()
    core = place_ref[0]
    left = left_ref[...]
    right = right_ref[...]
    cosine = turn_ref[0]
    sine = turn_ref[1]
    for pair in range(count // 2):
        if pair % 4 == 0:
            loads[3 + pair // 4].wait()
        signal = [jnp.concatenate([x_ref[0, 2 * pair + k], x_ref[1, 2 * pair + k]], 0) for k in (0, 1)]
        first = dot_nn(left, jnp.concatenate(signal, 1))
        turned = []
        for k in (0, 1):
            re = first[:128, 128 * k : 128 * k + 128]
            im = first[128:, 128 * k : 128 * k + 128]
            turned.append(
                jnp.concatenate(
                    [(re * cosine + im * sine).astype(BF16), (im * cosine - re * sine).astype(BF16)], 1
                )
            )
        final = dot_nt(right, jnp.concatenate(turned, 0))
        for k in (0, 1):
            stage[pl.ds(2 * pair + k, 256, stride=count), :] = final[:, 128 * k : 128 * k + 128]
    stores = []
    for chip in range(CHIPS):
        for rel in (0, 1):
            for t in range(8):
                row = pl.multiple_of(((2 * chip + (rel ^ core)) * 8 + t) * count, 8)
                value = stage[pl.ds(row, count), :].astype(BF16)
                if len(outs) == 1:
                    pack[chip, rel, :, 128 * t : 128 * t + 128] = value
                else:
                    outs[rel][chip, :, 128 * t : 128 * t + 128] = value
        if len(outs) == 1:
            stores.append(pltpu.make_async_copy(pack.at[chip], outs[0].at[chip], out_sems.at[chip]))
            stores[chip].start()
    for store in stores:
        store.wait()


def dft_part(place, signal, tables, count, lead):
    full = pltpu.HBM((CHIPS, 2, count, 1024), BF16)
    half = jax.ShapeDtypeStruct((CHIPS, count, 1024), BF16)
    shapes = (full,) if lead else (half, half)
    return pl.pallas_call(
        dft_kernel,
        in_specs=[SMEM] + [HBM] * 4,
        out_specs=(HBM,) if lead else (VMEM, VMEM),
        out_shape=shapes,
        scratch_shapes=[
            pltpu.VMEM((2, count, 128, 128), BF16),
            pltpu.VMEM((256, 256), BF16),
            pltpu.VMEM((2, 128, 128), F32),
            pltpu.VMEM((256, 256), BF16),
            pltpu.VMEM((256 * count, 128), F32),
            pltpu.SemaphoreType.DMA((3 + count // 8,)),
            pltpu.VMEM((CHIPS if lead else 1, 2, count, 1024), BF16),
            pltpu.SemaphoreType.DMA((CHIPS,)),
        ],
        compiler_params=params(60 if lead else 12),
        cost_estimate=cost(count << 25, count << 17),
        name="dft_lead" if lead else "dft_rest",
    )(place, signal, *tables)


def product(rows, cols):
    scale = 1.0 / NF
    real = dot_nt(rows, cols) * scale
    imag = (dot_nt(rows[:, HALF:], cols[:, :HALF]) - dot_nt(rows[:, :HALF], cols[:, HALF:])) * scale
    return real, imag


def gram_first_kernel(place_ref, kept_ref, swapped_ref, *rest):
    out_refs, full = rest[:N_TM], rest[N_TM]
    own = place_ref[1]
    sides = (kept_ref, swapped_ref)
    for a in (0, 1):
        for b in (0, 1):
            values = product(sides[a][...], sides[b][...])
            for q in (0, 1):
                full[q, a, :, SIDE_A * b : SIDE_A * b + SIDE_A] = values[q].astype(BF16)
    for k in range(N_TM):
        row = pl.multiple_of((own ^ k) * OWN_A, OWN_A)
        for q in (0, 1):
            for a in (0, 1):
                out_refs[k][q, OWN_A * a : OWN_A * a + OWN_A] = full[q, a, pl.ds(row, OWN_A), :]


def gram_first(place, kept, swapped):
    return pl.pallas_call(
        gram_first_kernel,
        in_specs=[SMEM, VMEM, VMEM],
        out_specs=(VMEM,) * N_TM,
        out_shape=(jax.ShapeDtypeStruct((2, 2 * OWN_A, COLS_A), BF16),) * N_TM,
        scratch_shapes=[pltpu.VMEM((2, 2, SIDE_A, COLS_A), BF16)],
        compiler_params=params(10),
        cost_estimate=cost(1 << 30, 6 << 20),
        name="gram_first",
    )(place, kept, swapped)


def gram_second_kernel(mine_ref, kept_ref, swapped_ref, out_hbm, out_ref, sems):
    mine = mine_ref[...]
    sides = [product(mine, kept_ref[...]), product(mine, swapped_ref[...])]
    second = product(mine, mine)
    copies = []
    for q in (0, 1):
        first = jnp.concatenate([sides[0][q], sides[1][q]], 1)
        flipped = first.T
        flipped = (-flipped if q else flipped).astype(BF16)
        blocks = [first[:, COLS_B * j : COLS_B * j + COLS_B].astype(BF16) for j in range(PIECES)]
        blocks.append(second[q].astype(BF16))
        rows = 2 * OWN_B
        for r in range(N_TM):
            for j in range(PIECES + 1):
                out_ref[r, q, rows * j : rows * j + rows, :] = blocks[j][rows * r : rows * r + rows]
            for a in (0, 1):
                row = (PIECES + 1) * rows + OWN_A * a
                src = SIDE_A * a + OWN_A * r
                out_ref[r, q, row : row + OWN_A, :] = flipped[src : src + OWN_A]
        copies.append(pltpu.make_async_copy(out_ref.at[:, q], out_hbm.at[:, q], sems.at[q]))
        copies[q].start()
    for copy in copies:
        copy.wait()


def gram_second(mine, kept, swapped):
    rows = 2 * (PIECES + 1) * OWN_B + 2 * OWN_A
    return pl.pallas_call(
        gram_second_kernel,
        in_specs=[VMEM, VMEM, VMEM],
        out_specs=HBM,
        out_shape=pltpu.HBM((N_TM, 2, rows, COLS_B), BF16),
        scratch_shapes=[
            pltpu.VMEM((N_TM, 2, rows, COLS_B), BF16),
            pltpu.SemaphoreType.DMA((2,)),
        ],
        compiler_params=params(14),
        cost_estimate=cost(1 << 29, 6 << 20),
        name="gram_second",
    )(mine, kept, swapped)


def placed(values, table):
    parts = []
    for value in values:
        high = value.astype(BF16)
        parts += [high, (value - high.astype(F32)).astype(BF16)]
    result = dot_nn(jnp.concatenate(parts, 0), table)
    size = values[0].shape[0]
    return [result[2 * k * size : (2 * k + 1) * size] + result[(2 * k + 1) * size : (2 * k + 2) * size] for k in range(len(values))]


def spread_kernel(*refs):
    terms, order_ref, out_ref = refs[:N_TM], refs[N_TM], refs[-1]
    totals = []
    for q in (0, 1):
        total = terms[0][q].astype(F32)
        for k in range(1, N_TM):
            total = total + terms[k][q].astype(F32)
        totals.append(total)
    spread = placed(totals, order_ref[:COLS_A, :])
    for q in (0, 1):
        out_ref[q] = spread[q]


def spread_first(terms, order):
    return pl.pallas_call(
        spread_kernel,
        in_specs=[VMEM] * (N_TM + 1),
        out_specs=VMEM,
        out_shape=jax.ShapeDtypeStruct((2, 2 * OWN_A, 1024), F32),
        compiler_params=params(8),
        cost_estimate=cost(1 << 28, 1 << 22),
        name="spread_first",
    )(*terms, order)


def finish_kernel(place_ref, terms_ref, base_ref, order_ref, out_ref):
    core = place_ref[0]
    rows = 2 * OWN_B
    last, extra = [], []
    for q in (0, 1):
        total = terms_ref[0, q].astype(F32)
        for t in range(1, N_TM):
            total = total + terms_ref[t, q].astype(F32)
        last.append(jnp.concatenate([total[rows * j : rows * j + rows] for j in range(PIECES + 1)], 1))
        extra.append(total[(PIECES + 1) * rows :])
    lower = placed(last, order_ref[...])
    upper = placed(extra, order_ref[COLS_A:, :])
    for q in (0, 1):
        top = base_ref[q] + upper[q]
        for rel in (0, 1):
            for chip in (0, 1):
                row = pl.multiple_of(64 * chip + 32 * (rel ^ core), 8)
                src = OWN_A * rel + FIRST * chip
                out_ref[q, pl.ds(row, FIRST), :] = top[src : src + FIRST]
                src = 2 * SECOND * chip + SECOND * rel
                out_ref[q, pl.ds(pl.multiple_of(row + FIRST, 8), SECOND), :] = lower[q][src : src + SECOND]


def finish(place, terms, base, order):
    return pl.pallas_call(
        finish_kernel,
        in_specs=[SMEM] + [VMEM] * 3,
        out_specs=VMEM,
        out_shape=jax.ShapeDtypeStruct((2, 128, 1024), F32),
        compiler_params=params(8),
        cost_estimate=cost(1 << 28, 1 << 22),
        name="finish",
    )(place, terms, base, order)


def weight_kernel(place_ref, *refs):
    blocks, out_ref, rows = refs[:N_TM], refs[N_TM], refs[-1]
    own, far, z = place_ref[1], place_ref[2], place_ref[3]
    for k in range(N_TM):
        source = (z - (own ^ k)) & 7
        for dx in (0, 1):
            chip = (far ^ dx) * 8 + source
            for dc in (0, 1):
                early = pl.multiple_of(dc * SIDE_A + chip * FIRST, 8)
                late = pl.multiple_of(COLS_A + chip * 2 * SECOND + dc * SECOND, 8)
                for p in (0, 1):
                    block = blocks[k][dc, dx, p].astype(F32)
                    rows[p, pl.ds(early, FIRST), :] = block[:FIRST]
                    rows[p, pl.ds(late, SECOND), :] = block[FIRST:]
    for p in (0, 1):
        flipped = rows[p].T
        straight = flipped.astype(BF16)
        out_ref[:256, 1024 * p : 1024 * p + 1024] = (-flipped).astype(BF16) if p else straight
        out_ref[256:, 1024 * (1 - p) : 1024 * (1 - p) + 1024] = straight


def weight_stack(place, blocks):
    return pl.pallas_call(
        weight_kernel,
        in_specs=[SMEM] + [VMEM] * N_TM,
        out_specs=VMEM,
        out_shape=jax.ShapeDtypeStruct((HALF, 2048), BF16),
        scratch_shapes=[pltpu.VMEM((2, 1024, 256), F32)],
        compiler_params=params(10),
        cost_estimate=cost(1 << 27, 1 << 22),
        name="weights",
    )(place, *blocks)


def beam_kernel(kept_ref, swapped_ref, second_ref, weight_ref, out_ref):
    total = None
    for p in (0, 1):
        lanes = slice(HALF * p, HALF * p + HALF)
        column = 1024 * p
        for ref in (kept_ref, swapped_ref, second_ref):
            count = ref.shape[0]
            term = dot_nn(weight_ref[:, column : column + count], ref[:, lanes])
            column += count
            total = term if total is None else total + term
    out_ref[...] = total.T.astype(BF16)


def beam_sum(kept, swapped, second, weights):
    return pl.pallas_call(
        beam_kernel,
        in_specs=[VMEM] * 4,
        out_specs=VMEM,
        out_shape=jax.ShapeDtypeStruct((HALF, HALF), BF16),
        compiler_params=params(10),
        cost_estimate=cost(1 << 29, 1 << 22),
        name="beams",
    )(kept, swapped, second, weights)


def swap(array, axis):
    return lax.ppermute(array, axis, [(0, 1), (1, 0)])


def with_partners(array):
    pairs = lambda k: [(i, i ^ k) for i in range(N_TM)]
    return [array] + [lax.ppermute(array, TM, pairs(k)) for k in range(1, N_TM)]


def to_partners(arrays):
    pairs = lambda k: [(i, i ^ k) for i in range(N_TM)]
    return [arrays[0]] + [lax.ppermute(arrays[k], TM, pairs(k)) for k in range(1, N_TM)]


def behind(value, other):
    return lax.optimization_barrier((value, other))[0]


def step(voltages, beam_weights):
    left, cosine, sine, right = dft_tables()
    tables = (jnp.asarray(left, BF16), jnp.asarray(np.stack([cosine, sine])), jnp.asarray(right, BF16))
    signal = voltages.reshape(2, 32, SPECTRA, 32, 128).transpose(0, 1, 3, 2, 4)
    signal = signal.reshape(2, 32, 128, 128)
    where = ("stat_2", TM, "stat_0", "stat_1")
    place = jnp.stack([lax.axis_index(a) for a in where]).astype(jnp.int32)

    spots = [(x, z, t) for x in (0, 1) for z in range(8) for t in range(N_TM)]
    at = lambda x, z, t: (x * 8 + z % 8) * N_TM + t
    rings = [[(at(x, z, t), at(x ^ dx, z + t, t)) for x, z, t in spots] for dx in (0, 1)]
    block = jnp.stack([lax.ppermute(beam_weights, (*CHIP, *TM), ring) for ring in rings])

    (ready_a,) = dft_part(place, signal, tables, FIRST, True)
    own_b, other_b = dft_part(place, signal, tables, SECOND, False)
    partner_b = swap(other_b, "stat_2")
    ready_b = jnp.concatenate([own_b, partner_b], 1)

    near = swap(block, "stat_2")
    block = jnp.stack([block, near])
    blocks_k = with_partners(block)
    columns = natural_columns(behind(lax.axis_index("stat_2"), ready_b))
    order = (columns[:, None] == jnp.arange(1024, dtype=jnp.int32)[None, :]).astype(BF16)

    arrived = lax.all_to_all(ready_a, CHIP, 0, 0, tiled=True)
    second = lax.all_to_all(ready_b, CHIP, 0, 0, tiled=True).reshape(COLS_B, 1024)
    kept = arrived[:, 0].reshape(SIDE_A, 1024)
    other = arrived[:, 1].reshape(SIDE_A, 1024)
    swapped = swap(other, "stat_2")
    terms = gram_first(place, kept, swapped)
    terms = to_partners(terms)
    blocks = gram_second(second, kept, swapped)
    last = lax.all_to_all(blocks, TM, 0, 0, tiled=True)

    weights = weight_stack(place, blocks_k)
    beams = beam_sum(kept, swapped, second, weights)
    beams = beams.reshape(NF // 32, SPECTRA, 2, 256)
    base = spread_first(terms, order)
    rows = finish(place, last, base, order)
    return beams, rows.transpose(1, 0, 2)[:, None]


def solution(mesh):
    finer = Mesh(
        mesh.devices.reshape(2, 8, 2, 4, 2), ("stat_0", "stat_1", "stat_2", "tm_0", "tm_1")
    )
    return jax.shard_map(
        step,
        mesh=finer,
        in_specs=(P(None, STAT, TM, None), P(None, STAT, None)),
        out_specs=(P(STAT, TM, None, None), P(TM, STAT, None, None)),
        check_vma=False,
    )
```

```python
import math

import jax
import jax.numpy as jnp
import numpy as np
from jax import lax
from jax.experimental import pallas as pl
from jax.experimental.pallas import tpu as pltpu
from jax.sharding import Mesh
from jax.sharding import PartitionSpec as P


STAT = ("stat_0", "stat_1", "stat_2")
CHIP = ("stat_0", "stat_1")
TM = ("tm_0", "tm_1")
NF = 4096
CHIPS = 16
N_TM = 8
SPECTRA = 4
FIRST, SECOND = 16, 16
SIDE_A, SIDE_B = CHIPS * FIRST, CHIPS * SECOND
OWN_A, OWN_B = SIDE_A // N_TM, SIDE_B // N_TM
COLS_A, COLS_B = 2 * SIDE_A, 2 * SIDE_B
ROWS_B = 2 * OWN_B
HALF = 512
BF16 = jnp.bfloat16
F32 = jnp.float32
VMEM = pl.BlockSpec(memory_space=pltpu.VMEM)
SMEM = pl.BlockSpec(memory_space=pltpu.SMEM)
ANY = pl.BlockSpec(memory_space=pl.ANY)
HBM = pl.BlockSpec(memory_space=pltpu.HBM)


def rotation(angle):
    cosine, sine = np.cos(angle), np.sin(angle)
    return np.block([[cosine, sine], [-sine, cosine]])


def dft_tables():
    outer = np.arange(32)
    angle = 2.0 * np.pi * np.outer(outer, outer) / 32
    eye = np.eye(SPECTRA)
    spread = lambda m: np.einsum("wc,st->wsct", m, eye).reshape(128, 128)
    cosine, sine = spread(np.cos(angle)), spread(np.sin(angle))
    left = np.block([[cosine, sine], [-sine, cosine]])
    w0 = np.repeat(np.arange(32), SPECTRA)
    twist = 2.0 * np.pi * np.outer(w0, np.arange(128)) / NF
    inner = 2.0 * np.pi * np.outer(np.arange(128), np.arange(128)) / 128
    right = rotation(inner) / math.sqrt(NF)
    right = right.reshape(2, 32, 4, 256).transpose(1, 0, 2, 3).reshape(256, 256)
    return (
        left.astype(np.float32),
        np.cos(twist).astype(np.float32),
        np.sin(twist).astype(np.float32),
        right.astype(np.float32),
    )


def natural_columns(core):
    def of(core):
        rel, chip, item = np.meshgrid(np.arange(2), np.arange(CHIPS), np.arange(32), indexing="ij")
        place = 32 * (2 * chip + (rel ^ core)) + item
        late = place[:, :, FIRST:].transpose(1, 0, 2)
        return np.concatenate([place[:, :, :FIRST].reshape(-1), late.reshape(-1)]).astype(np.int32)

    return jnp.where(core == 0, jnp.asarray(of(0)), jnp.asarray(of(1)))


def params(mib):
    return pltpu.CompilerParams(vmem_limit_bytes=mib * 1024 * 1024)


def cost(macs, moved):
    return pl.CostEstimate(flops=2 * macs, bytes_accessed=moved, transcendentals=0)


def dot_nn(a, b):
    return lax.dot_general(a, b, (((1,), (0,)), ((), ())), preferred_element_type=F32)


def dot_nt(a, b):
    return lax.dot_general(a, b, (((1,), (1,)), ((), ())), preferred_element_type=F32)


def dft_kernel(place_ref, x_hbm, left_hbm, turn_hbm, right_hbm, *refs):
    outs, (x_ref, left_ref, turn_ref, right_ref, stage, sems, pack, out_sems) = refs[:-8], refs[-8:]
    count = x_ref.shape[1]
    start = 0 if len(outs) == 1 else FIRST
    loads = [
        pltpu.make_async_copy(left_hbm, left_ref, sems.at[0]),
        pltpu.make_async_copy(turn_hbm, turn_ref, sems.at[1]),
        pltpu.make_async_copy(right_hbm, right_ref, sems.at[2]),
    ]
    groups = count // 8
    for g in range(groups):
        loads.append(
            pltpu.make_async_copy(
                x_hbm.at[:, start + 8 * g : start + 8 * g + 8], x_ref.at[:, 8 * g : 8 * g + 8], sems.at[3 + g]
            )
        )
    for load in [loads[0], loads[3], *loads[1:3], *loads[4:]]:
        load.start()
    for load in loads[:3]:
        load.wait()
    core = place_ref[0]
    left = left_ref[...]
    right = right_ref[...]
    cosine = turn_ref[0]
    sine = turn_ref[1]
    for pair in range(count // 2):
        if pair % 4 == 0:
            loads[3 + pair // 4].wait()
        signal = [jnp.concatenate([x_ref[0, 2 * pair + k], x_ref[1, 2 * pair + k]], 0) for k in (0, 1)]
        first = dot_nn(left, jnp.concatenate(signal, 1))
        turned = []
        for k in (0, 1):
            re = first[:128, 128 * k : 128 * k + 128]
            im = first[128:, 128 * k : 128 * k + 128]
            turned.append(
                jnp.concatenate(
                    [(re * cosine + im * sine).astype(BF16), (im * cosine - re * sine).astype(BF16)], 1
                )
            )
        final = dot_nt(right, jnp.concatenate(turned, 0))
        for k in (0, 1):
            stage[pl.ds(2 * pair + k, 256, stride=count), :] = final[:, 128 * k : 128 * k + 128]
    stores = []
    for chip in range(CHIPS):
        for rel in (0, 1):
            for t in range(8):
                row = pl.multiple_of(((2 * chip + (rel ^ core)) * 8 + t) * count, 8)
                value = stage[pl.ds(row, count), :].astype(BF16)
                if len(outs) == 1:
                    pack[chip, rel, :, 128 * t : 128 * t + 128] = value
                else:
                    outs[rel][chip, :, 128 * t : 128 * t + 128] = value
        if len(outs) == 1:
            stores.append(pltpu.make_async_copy(pack.at[chip], outs[0].at[chip], out_sems.at[chip]))
            stores[chip].start()
    for store in stores:
        store.wait()


def dft_part(place, signal, tables, count, lead):
    full = pltpu.HBM((CHIPS, 2, count, 1024), BF16)
    half = jax.ShapeDtypeStruct((CHIPS, count, 1024), BF16)
    shapes = (full,) if lead else (half, half)
    return pl.pallas_call(
        dft_kernel,
        in_specs=[SMEM] + [HBM] * 4,
        out_specs=(HBM,) if lead else (VMEM, VMEM),
        out_shape=shapes,
        scratch_shapes=[
            pltpu.VMEM((2, count, 128, 128), BF16),
            pltpu.VMEM((256, 256), BF16),
            pltpu.VMEM((2, 128, 128), F32),
            pltpu.VMEM((256, 256), BF16),
            pltpu.VMEM((256 * count, 128), F32),
            pltpu.SemaphoreType.DMA((3 + count // 8,)),
            pltpu.VMEM((CHIPS if lead else 1, 2, count, 1024), BF16),
            pltpu.SemaphoreType.DMA((CHIPS,)),
        ],
        compiler_params=params(60 if lead else 12),
        cost_estimate=cost(count << 25, count << 17),
        name="dft_lead" if lead else "dft_rest",
    )(place, signal, *tables)


def product(rows, cols):
    scale = 1.0 / NF
    real = dot_nt(rows, cols) * scale
    imag = (dot_nt(rows[:, HALF:], cols[:, :HALF]) - dot_nt(rows[:, :HALF], cols[:, HALF:])) * scale
    return real, imag


def gram_first_kernel(place_ref, kept_ref, swapped_ref, *rest):
    out_refs, full = rest[:N_TM], rest[N_TM]
    own = place_ref[1]
    sides = (kept_ref, swapped_ref)
    for a in (0, 1):
        for b in (0, 1):
            values = product(sides[a][...], sides[b][...])
            for q in (0, 1):
                full[q, a, :, SIDE_A * b : SIDE_A * b + SIDE_A] = values[q].astype(BF16)
    for k in range(N_TM):
        row = pl.multiple_of((own ^ k) * OWN_A, OWN_A)
        for q in (0, 1):
            for a in (0, 1):
                out_refs[k][q, OWN_A * a : OWN_A * a + OWN_A] = full[q, a, pl.ds(row, OWN_A), :]


def gram_first(place, kept, swapped):
    return pl.pallas_call(
        gram_first_kernel,
        in_specs=[SMEM, VMEM, VMEM],
        out_specs=(VMEM,) * N_TM,
        out_shape=(jax.ShapeDtypeStruct((2, 2 * OWN_A, COLS_A), BF16),) * N_TM,
        scratch_shapes=[pltpu.VMEM((2, 2, SIDE_A, COLS_A), BF16)],
        compiler_params=params(10),
        cost_estimate=cost(1 << 30, 6 << 20),
        name="gram_first",
    )(place, kept, swapped)


def gram_late_kernel(mine_ref, *refs):
    col_refs, (out_hbm, out_ref, sems) = refs[:-3], refs[-3:]
    mine = mine_ref[...]
    sides = [product(mine, ref[...]) for ref in (col_refs or (mine_ref,))]
    copies = []
    for q in (0, 1):
        start = 0
        for side in sides:
            value = side[q].astype(BF16)
            width = value.shape[1]
            for r in range(N_TM):
                out_ref[r, q, :, start : start + width] = value[ROWS_B * r : ROWS_B * r + ROWS_B]
            start += width
        copies.append(pltpu.make_async_copy(out_ref.at[:, q], out_hbm.at[:, q], sems.at[q]))
        copies[q].start()
    for copy in copies:
        copy.wait()


def gram_late(mine, *others):
    width = COLS_A if others else COLS_B
    shape = (N_TM, 2, ROWS_B, width)
    return pl.pallas_call(
        gram_late_kernel,
        in_specs=[VMEM] * (1 + len(others)),
        out_specs=HBM,
        out_shape=pltpu.HBM(shape, BF16),
        scratch_shapes=[pltpu.VMEM(shape, BF16), pltpu.SemaphoreType.DMA((2,))],
        compiler_params=params(10),
        cost_estimate=cost(1 << 29, 4 << 20),
        name="gram_cross" if others else "gram_second",
    )(mine, *others)


def mirror_kernel(place_ref, terms_ref, sums_ref, *refs):
    mirror_refs, flip = refs[:N_TM], refs[N_TM]
    own = place_ref[1]
    for q in (0, 1):
        total = terms_ref[0, q].astype(F32)
        for t in range(1, N_TM):
            total = total + terms_ref[t, q].astype(F32)
        sums_ref[q] = total
        block = jnp.concatenate([-total if q else total, jnp.zeros((128 - ROWS_B, COLS_A), F32)], 0)
        flip[q] = block.T
        for k in range(N_TM):
            for a in (0, 1):
                row = pl.multiple_of(SIDE_A * a + (own ^ k) * OWN_A, OWN_A)
                mirror_refs[k][q, OWN_A * a : OWN_A * a + OWN_A] = flip[q, pl.ds(row, OWN_A), :].astype(BF16)


def mirror(place, terms):
    return pl.pallas_call(
        mirror_kernel,
        in_specs=[SMEM, VMEM],
        out_specs=(VMEM,) * (N_TM + 1),
        out_shape=(jax.ShapeDtypeStruct((2, ROWS_B, COLS_A), F32),)
        + (jax.ShapeDtypeStruct((2, 2 * OWN_A, 128), BF16),) * N_TM,
        scratch_shapes=[pltpu.VMEM((2, COLS_A, 128), F32)],
        compiler_params=params(8),
        cost_estimate=cost(1 << 27, 1 << 21),
        name="mirror",
    )(place, terms)


def placed(values, table):
    parts = []
    for value in values:
        high = value.astype(BF16)
        parts += [high, (value - high.astype(F32)).astype(BF16)]
    result = dot_nn(jnp.concatenate(parts, 0), table)
    size = values[0].shape[0]
    return [result[2 * k * size : (2 * k + 1) * size] + result[(2 * k + 1) * size : (2 * k + 2) * size] for k in range(len(values))]


def spread_kernel(*refs):
    terms, order_ref, out_ref = refs[:N_TM], refs[N_TM], refs[-1]
    totals = []
    for q in (0, 1):
        total = terms[0][q].astype(F32)
        for k in range(1, N_TM):
            total = total + terms[k][q].astype(F32)
        totals.append(total)
    spread = placed(totals, order_ref[:COLS_A, :])
    for q in (0, 1):
        out_ref[q] = spread[q]


def spread_first(terms, order):
    return pl.pallas_call(
        spread_kernel,
        in_specs=[VMEM] * (N_TM + 1),
        out_specs=VMEM,
        out_shape=jax.ShapeDtypeStruct((2, 2 * OWN_A, 1024), F32),
        compiler_params=params(8),
        cost_estimate=cost(1 << 28, 1 << 22),
        name="spread_first",
    )(*terms, order)


def cross_kernel(place_ref, base_ref, sums_ref, order_ref, *refs):
    mirrors, out_ref = refs[:N_TM], refs[-1]
    core, own = place_ref[0], place_ref[1]
    spread = placed([sums_ref[0], sums_ref[1]], order_ref[:COLS_A, :])
    item = lax.broadcasted_iota(jnp.int32, (128, 128), 0)
    lane = lax.broadcasted_iota(jnp.int32, (128, 128), 1)
    chip, rel = item // (2 * SECOND), item // SECOND % 2
    target = 64 * chip + 32 * (rel ^ core) + FIRST + item % SECOND
    narrow = jnp.where((target == lane) & (item < ROWS_B), 1.0, 0.0).astype(BF16)
    for q in (0, 1):
        out_ref[q, : 2 * OWN_A, :] = base_ref[q]
        out_ref[q, 2 * OWN_A :, :] = spread[q]
        for k in range(N_TM):
            col = pl.multiple_of((own ^ k) * 128, 128)
            out_ref[q, : 2 * OWN_A, pl.ds(col, 128)] += dot_nn(mirrors[k][q], narrow)


def spread_cross(place, base, sums, order, mirrors):
    return pl.pallas_call(
        cross_kernel,
        in_specs=[SMEM] + [VMEM] * (N_TM + 3),
        out_specs=VMEM,
        out_shape=jax.ShapeDtypeStruct((2, 128, 1024), F32),
        compiler_params=params(8),
        cost_estimate=cost(1 << 28, 1 << 22),
        name="spread_cross",
    )(place, base, sums, order, *mirrors)


def finish_kernel(place_ref, terms_ref, base_ref, order_ref, out_ref):
    core = place_ref[0]
    totals = []
    for q in (0, 1):
        total = terms_ref[0, q].astype(F32)
        for t in range(1, N_TM):
            total = total + terms_ref[t, q].astype(F32)
        totals.append(total)
    lower = placed(totals, order_ref[COLS_A:, :])
    for q in (0, 1):
        low = base_ref[q, 2 * OWN_A :, :] + lower[q]
        for rel in (0, 1):
            for chip in (0, 1):
                row = pl.multiple_of(64 * chip + 32 * (rel ^ core), 8)
                src = OWN_A * rel + FIRST * chip
                out_ref[q, pl.ds(row, FIRST), :] = base_ref[q, src : src + FIRST, :]
                src = 2 * SECOND * chip + SECOND * rel
                out_ref[q, pl.ds(pl.multiple_of(row + FIRST, 8), SECOND), :] = low[src : src + SECOND]


def finish(place, terms, base, order):
    return pl.pallas_call(
        finish_kernel,
        in_specs=[SMEM] + [VMEM] * 3,
        out_specs=VMEM,
        out_shape=jax.ShapeDtypeStruct((2, 128, 1024), F32),
        compiler_params=params(8),
        cost_estimate=cost(1 << 28, 1 << 22),
        name="finish",
    )(place, terms, base, order)


def weight_kernel(place_ref, *refs):
    blocks, out_ref, rows = refs[:N_TM], refs[N_TM], refs[-1]
    own, far, z = place_ref[1], place_ref[2], place_ref[3]
    for k in range(N_TM):
        source = (z - (own ^ k)) & 7
        for dx in (0, 1):
            chip = (far ^ dx) * 8 + source
            for dc in (0, 1):
                early = pl.multiple_of(dc * SIDE_A + chip * FIRST, 8)
                late = pl.multiple_of(COLS_A + chip * 2 * SECOND + dc * SECOND, 8)
                for p in (0, 1):
                    block = blocks[k][dc, dx, p].astype(F32)
                    rows[p, pl.ds(early, FIRST), :] = block[:FIRST]
                    rows[p, pl.ds(late, SECOND), :] = block[FIRST:]
    for p in (0, 1):
        flipped = rows[p].T
        straight = flipped.astype(BF16)
        out_ref[:256, 1024 * p : 1024 * p + 1024] = (-flipped).astype(BF16) if p else straight
        out_ref[256:, 1024 * (1 - p) : 1024 * (1 - p) + 1024] = straight


def weight_stack(place, blocks):
    return pl.pallas_call(
        weight_kernel,
        in_specs=[SMEM] + [VMEM] * N_TM,
        out_specs=VMEM,
        out_shape=jax.ShapeDtypeStruct((HALF, 2048), BF16),
        scratch_shapes=[pltpu.VMEM((2, 1024, 256), F32)],
        compiler_params=params(10),
        cost_estimate=cost(1 << 27, 1 << 22),
        name="weights",
    )(place, *blocks)


def beam_kernel(kept_ref, swapped_ref, second_ref, weight_ref, out_ref):
    total = None
    for p in (0, 1):
        lanes = slice(HALF * p, HALF * p + HALF)
        column = 1024 * p
        for ref in (kept_ref, swapped_ref, second_ref):
            count = ref.shape[0]
            term = dot_nn(weight_ref[:, column : column + count], ref[:, lanes])
            column += count
            total = term if total is None else total + term
    out_ref[...] = total.T.astype(BF16)


def beam_sum(kept, swapped, second, weights):
    return pl.pallas_call(
        beam_kernel,
        in_specs=[VMEM] * 4,
        out_specs=VMEM,
        out_shape=jax.ShapeDtypeStruct((HALF, HALF), BF16),
        compiler_params=params(10),
        cost_estimate=cost(1 << 29, 1 << 22),
        name="beams",
    )(kept, swapped, second, weights)


def swap(array, axis):
    return lax.ppermute(array, axis, [(0, 1), (1, 0)])


def with_partners(array):
    pairs = lambda k: [(i, i ^ k) for i in range(N_TM)]
    return [array] + [lax.ppermute(array, TM, pairs(k)) for k in range(1, N_TM)]


def to_partners(arrays):
    pairs = lambda k: [(i, i ^ k) for i in range(N_TM)]
    return [arrays[0]] + [lax.ppermute(arrays[k], TM, pairs(k)) for k in range(1, N_TM)]


def behind(value, other):
    return lax.optimization_barrier((value, other))[0]


def step(voltages, beam_weights):
    left, cosine, sine, right = dft_tables()
    tables = (jnp.asarray(left, BF16), jnp.asarray(np.stack([cosine, sine])), jnp.asarray(right, BF16))
    signal = voltages.reshape(2, 32, SPECTRA, 32, 128).transpose(0, 1, 3, 2, 4)
    signal = signal.reshape(2, 32, 128, 128)
    where = ("stat_2", TM, "stat_0", "stat_1")
    place = jnp.stack([lax.axis_index(a) for a in where]).astype(jnp.int32)

    spots = [(x, z, t) for x in (0, 1) for z in range(8) for t in range(N_TM)]
    at = lambda x, z, t: (x * 8 + z % 8) * N_TM + t
    rings = [[(at(x, z, t), at(x ^ dx, z + t, t)) for x, z, t in spots] for dx in (0, 1)]
    block = jnp.stack([lax.ppermute(beam_weights, (*CHIP, *TM), ring) for ring in rings])

    (ready_a,) = dft_part(place, signal, tables, FIRST, True)
    own_b, other_b = dft_part(place, signal, tables, SECOND, False)
    partner_b = swap(other_b, "stat_2")
    ready_b = jnp.concatenate([own_b, partner_b], 1)

    near = swap(block, "stat_2")
    block = jnp.stack([block, near])
    blocks_k = with_partners(block)
    columns = natural_columns(behind(lax.axis_index("stat_2"), ready_b))
    order = (columns[:, None] == jnp.arange(1024, dtype=jnp.int32)[None, :]).astype(BF16)

    arrived = lax.all_to_all(ready_a, CHIP, 0, 0, tiled=True)
    second = lax.all_to_all(ready_b, CHIP, 0, 0, tiled=True).reshape(COLS_B, 1024)
    kept = arrived[:, 0].reshape(SIDE_A, 1024)
    other = arrived[:, 1].reshape(SIDE_A, 1024)
    swapped = swap(other, "stat_2")
    terms = gram_first(place, kept, swapped)
    terms = to_partners(terms)
    cross = gram_late(second, kept, swapped)
    cross = lax.all_to_all(cross, TM, 0, 0, tiled=True)
    late = gram_late(second)
    late = lax.all_to_all(late, TM, 0, 0, tiled=True)

    weights = weight_stack(place, blocks_k)
    beams = beam_sum(kept, swapped, second, weights)
    beams = beams.reshape(NF // 32, SPECTRA, 2, 256)
    base = spread_first(terms, order)
    sums, *mirrors = mirror(place, cross)
    mirrors = to_partners(mirrors)
    base = spread_cross(place, base, sums, order, mirrors)
    rows = finish(place, late, base, order)
    return beams, rows.transpose(1, 0, 2)[:, None]


def solution(mesh):
    finer = Mesh(
        mesh.devices.reshape(2, 8, 2, 4, 2), ("stat_0", "stat_1", "stat_2", "tm_0", "tm_1")
    )
    return jax.shard_map(
        step,
        mesh=finer,
        in_specs=(P(None, STAT, TM, None), P(None, STAT, None)),
        out_specs=(P(STAT, TM, None, None), P(TM, STAT, None, None)),
        check_vma=False,
    )
```

```python
import math

import jax
import jax.numpy as jnp
import numpy as np
from jax import lax
from jax.experimental import pallas as pl
from jax.experimental.pallas import tpu as pltpu
from jax.sharding import Mesh
from jax.sharding import PartitionSpec as P


STAT = ("stat_0", "stat_1", "stat_2")
CHIP = ("stat_0", "stat_1")
TM = ("tm_0", "tm_1")
NF = 4096
CHIPS = 16
N_TM = 8
SPECTRA = 4
FIRST, SECOND = 16, 16
SIDE_A, SIDE_B = CHIPS * FIRST, CHIPS * SECOND
OWN_A, OWN_B = SIDE_A // N_TM, SIDE_B // N_TM
COLS_A, COLS_B = 2 * SIDE_A, 2 * SIDE_B
PIECES = COLS_A // COLS_B
HALF = 512
BF16 = jnp.bfloat16
F32 = jnp.float32
VMEM = pl.BlockSpec(memory_space=pltpu.VMEM)
SMEM = pl.BlockSpec(memory_space=pltpu.SMEM)
ANY = pl.BlockSpec(memory_space=pl.ANY)
HBM = pl.BlockSpec(memory_space=pltpu.HBM)


def rotation(angle):
    cosine, sine = np.cos(angle), np.sin(angle)
    return np.block([[cosine, sine], [-sine, cosine]])


def dft_tables():
    outer = np.arange(32)
    angle = 2.0 * np.pi * np.outer(outer, outer) / 32
    eye = np.eye(SPECTRA)
    spread = lambda m: np.einsum("wc,st->wsct", m, eye).reshape(128, 128)
    cosine, sine = spread(np.cos(angle)), spread(np.sin(angle))
    left = np.block([[cosine, sine], [-sine, cosine]])
    w0 = np.repeat(np.arange(32), SPECTRA)
    twist = 2.0 * np.pi * np.outer(w0, np.arange(128)) / NF
    inner = 2.0 * np.pi * np.outer(np.arange(128), np.arange(128)) / 128
    right = rotation(inner) / math.sqrt(NF)
    right = right.reshape(2, 32, 4, 256).transpose(1, 0, 2, 3).reshape(256, 256)
    return (
        left.astype(np.float32),
        np.cos(twist).astype(np.float32),
        np.sin(twist).astype(np.float32),
        right.astype(np.float32),
    )


def natural_columns(core):
    def of(core):
        rel, chip, item = np.meshgrid(np.arange(2), np.arange(CHIPS), np.arange(32), indexing="ij")
        place = 32 * (2 * chip + (rel ^ core)) + item
        late = place[:, :, FIRST:].transpose(1, 0, 2)
        return np.concatenate([place[:, :, :FIRST].reshape(-1), late.reshape(-1)]).astype(np.int32)

    return jnp.where(core == 0, jnp.asarray(of(0)), jnp.asarray(of(1)))


def params(mib):
    return pltpu.CompilerParams(vmem_limit_bytes=mib * 1024 * 1024)


def cost(macs, moved):
    return pl.CostEstimate(flops=2 * macs, bytes_accessed=moved, transcendentals=0)


def dot_nn(a, b):
    return lax.dot_general(a, b, (((1,), (0,)), ((), ())), preferred_element_type=F32)


def dot_nt(a, b):
    return lax.dot_general(a, b, (((1,), (1,)), ((), ())), preferred_element_type=F32)


def dft_kernel(place_ref, x_hbm, left_hbm, turn_hbm, right_hbm, *refs):
    outs, (x_ref, left_ref, turn_ref, right_ref, stage, sems, pack, out_sems) = refs[:-8], refs[-8:]
    count = x_ref.shape[1]
    start = 0 if len(outs) == 1 else FIRST
    loads = [
        pltpu.make_async_copy(left_hbm, left_ref, sems.at[0]),
        pltpu.make_async_copy(turn_hbm, turn_ref, sems.at[1]),
        pltpu.make_async_copy(right_hbm, right_ref, sems.at[2]),
    ]
    groups = count // 8
    for g in range(groups):
        loads.append(
            pltpu.make_async_copy(
                x_hbm.at[:, start + 8 * g : start + 8 * g + 8], x_ref.at[:, 8 * g : 8 * g + 8], sems.at[3 + g]
            )
        )
    for load in [loads[0], loads[3], *loads[1:3], *loads[4:]]:
        load.start()
    for load in loads[:3]:
        load.wait()
    core = place_ref[0]
    left = left_ref[...]
    right = right_ref[...]
    cosine = turn_ref[0]
    sine = turn_ref[1]
    for pair in range(count // 2):
        if pair % 4 == 0:
            loads[3 + pair // 4].wait()
        signal = [jnp.concatenate([x_ref[0, 2 * pair + k], x_ref[1, 2 * pair + k]], 0) for k in (0, 1)]
        first = dot_nn(left, jnp.concatenate(signal, 1))
        turned = []
        for k in (0, 1):
            re = first[:128, 128 * k : 128 * k + 128]
            im = first[128:, 128 * k : 128 * k + 128]
            turned.append(
                jnp.concatenate(
                    [(re * cosine + im * sine).astype(BF16), (im * cosine - re * sine).astype(BF16)], 1
                )
            )
        final = dot_nt(right, jnp.concatenate(turned, 0))
        for k in (0, 1):
            stage[pl.ds(2 * pair + k, 256, stride=count), :] = final[:, 128 * k : 128 * k + 128]
    stores = []
    for chip in range(CHIPS):
        for rel in (0, 1):
            for t in range(8):
                row = pl.multiple_of(((2 * chip + (rel ^ core)) * 8 + t) * count, 8)
                value = stage[pl.ds(row, count), :].astype(BF16)
                if len(outs) == 1:
                    pack[chip, rel, :, 128 * t : 128 * t + 128] = value
                else:
                    outs[rel][chip, :, 128 * t : 128 * t + 128] = value
        if len(outs) == 1:
            stores.append(pltpu.make_async_copy(pack.at[chip], outs[0].at[chip], out_sems.at[chip]))
            stores[chip].start()
    for store in stores:
        store.wait()


def dft_part(place, signal, tables, count, lead):
    full = pltpu.HBM((CHIPS, 2, count, 1024), BF16)
    half = jax.ShapeDtypeStruct((CHIPS, count, 1024), BF16)
    shapes = (full,) if lead else (half, half)
    return pl.pallas_call(
        dft_kernel,
        in_specs=[SMEM] + [HBM] * 4,
        out_specs=(HBM,) if lead else (VMEM, VMEM),
        out_shape=shapes,
        scratch_shapes=[
            pltpu.VMEM((2, count, 128, 128), BF16),
            pltpu.VMEM((256, 256), BF16),
            pltpu.VMEM((2, 128, 128), F32),
            pltpu.VMEM((256, 256), BF16),
            pltpu.VMEM((256 * count, 128), F32),
            pltpu.SemaphoreType.DMA((3 + count // 8,)),
            pltpu.VMEM((CHIPS if lead else 1, 2, count, 1024), BF16),
            pltpu.SemaphoreType.DMA((CHIPS,)),
        ],
        compiler_params=params(60 if lead else 12),
        cost_estimate=cost(count << 25, count << 17),
        name="dft_lead" if lead else "dft_rest",
    )(place, signal, *tables)


def product(rows, cols):
    scale = 1.0 / NF
    real = dot_nt(rows, cols) * scale
    imag = (dot_nt(rows[:, HALF:], cols[:, :HALF]) - dot_nt(rows[:, :HALF], cols[:, HALF:])) * scale
    return real, imag


def gram_first_kernel(place_ref, kept_ref, swapped_ref, *rest):
    out_refs, full = rest[:N_TM], rest[N_TM]
    own = place_ref[1]
    sides = (kept_ref, swapped_ref)
    for a in (0, 1):
        for b in (0, 1):
            values = product(sides[a][...], sides[b][...])
            for q in (0, 1):
                full[q, a, :, SIDE_A * b : SIDE_A * b + SIDE_A] = values[q].astype(BF16)
    for k in range(N_TM):
        row = pl.multiple_of((own ^ k) * OWN_A, OWN_A)
        for q in (0, 1):
            for a in (0, 1):
                out_refs[k][q, OWN_A * a : OWN_A * a + OWN_A] = full[q, a, pl.ds(row, OWN_A), :]


def gram_first(place, kept, swapped):
    return pl.pallas_call(
        gram_first_kernel,
        in_specs=[SMEM, VMEM, VMEM],
        out_specs=(VMEM,) * N_TM,
        out_shape=(jax.ShapeDtypeStruct((2, 2 * OWN_A, COLS_A), BF16),) * N_TM,
        scratch_shapes=[pltpu.VMEM((2, 2, SIDE_A, COLS_A), BF16)],
        compiler_params=params(10),
        cost_estimate=cost(1 << 30, 6 << 20),
        name="gram_first",
    )(place, kept, swapped)


def gram_second_kernel(mine_ref, kept_ref, swapped_ref, out_hbm, out_ref, sems):
    mine = mine_ref[...]
    sides = [product(mine, kept_ref[...]), product(mine, swapped_ref[...])]
    second = product(mine, mine)
    copies = []
    for q in (0, 1):
        first = jnp.concatenate([sides[0][q], sides[1][q]], 1)
        flipped = first.T
        flipped = (-flipped if q else flipped).astype(BF16)
        blocks = [first[:, COLS_B * j : COLS_B * j + COLS_B].astype(BF16) for j in range(PIECES)]
        blocks.append(second[q].astype(BF16))
        rows = 2 * OWN_B
        for r in range(N_TM):
            for j in range(PIECES + 1):
                out_ref[r, q, rows * j : rows * j + rows, :] = blocks[j][rows * r : rows * r + rows]
            for a in (0, 1):
                row = (PIECES + 1) * rows + OWN_A * a
                src = SIDE_A * a + OWN_A * r
                out_ref[r, q, row : row + OWN_A, :] = flipped[src : src + OWN_A]
        copies.append(pltpu.make_async_copy(out_ref.at[:, q], out_hbm.at[:, q], sems.at[q]))
        copies[q].start()
    for copy in copies:
        copy.wait()


def gram_second(mine, kept, swapped):
    rows = 2 * (PIECES + 1) * OWN_B + 2 * OWN_A
    return pl.pallas_call(
        gram_second_kernel,
        in_specs=[VMEM, VMEM, VMEM],
        out_specs=HBM,
        out_shape=pltpu.HBM((N_TM, 2, rows, COLS_B), BF16),
        scratch_shapes=[
            pltpu.VMEM((N_TM, 2, rows, COLS_B), BF16),
            pltpu.SemaphoreType.DMA((2,)),
        ],
        compiler_params=params(14),
        cost_estimate=cost(1 << 29, 6 << 20),
        name="gram_second",
    )(mine, kept, swapped)


def placed(values, table):
    parts = []
    for value in values:
        high = value.astype(BF16)
        parts += [high, (value - high.astype(F32)).astype(BF16)]
    result = dot_nn(jnp.concatenate(parts, 0), table)
    size = values[0].shape[0]
    return [result[2 * k * size : (2 * k + 1) * size] + result[(2 * k + 1) * size : (2 * k + 2) * size] for k in range(len(values))]


def spread_kernel(*refs):
    terms, order_ref, out_ref = refs[:N_TM], refs[N_TM], refs[-1]
    totals = []
    for q in (0, 1):
        total = terms[0][q].astype(F32)
        for k in range(1, N_TM):
            total = total + terms[k][q].astype(F32)
        totals.append(total)
    spread = placed(totals, order_ref[:COLS_A, :])
    for q in (0, 1):
        out_ref[q] = spread[q]


def spread_first(terms, order):
    return pl.pallas_call(
        spread_kernel,
        in_specs=[VMEM] * (N_TM + 1),
        out_specs=VMEM,
        out_shape=jax.ShapeDtypeStruct((2, 2 * OWN_A, 1024), F32),
        compiler_params=params(8),
        cost_estimate=cost(1 << 28, 1 << 22),
        name="spread_first",
    )(*terms, order)


def finish_kernel(place_ref, terms_hbm, base_ref, order_ref, out_ref, terms_ref, sems):
    loads = [pltpu.make_async_copy(terms_hbm.at[:, q], terms_ref.at[:, q], sems.at[q]) for q in (0, 1)]
    for load in loads:
        load.start()
    core = place_ref[0]
    rows = 2 * OWN_B
    for q in (0, 1):
        loads[q].wait()
        total = terms_ref[0, q].astype(F32)
        for t in range(1, N_TM):
            total = total + terms_ref[t, q].astype(F32)
        last = jnp.concatenate([total[rows * j : rows * j + rows] for j in range(PIECES + 1)], 1)
        (low,) = placed([last], order_ref[...])
        (extra,) = placed([total[(PIECES + 1) * rows :]], order_ref[COLS_A:, :])
        top = base_ref[q] + extra
        for rel in (0, 1):
            for chip in (0, 1):
                row = pl.multiple_of(64 * chip + 32 * (rel ^ core), 8)
                src = OWN_A * rel + FIRST * chip
                out_ref[pl.ds(row, FIRST), q, :] = top[src : src + FIRST]
                src = 2 * SECOND * chip + SECOND * rel
                out_ref[pl.ds(row + FIRST, SECOND), q, :] = low[src : src + SECOND]


def finish(place, terms, base, order):
    return pl.pallas_call(
        finish_kernel,
        in_specs=[SMEM, HBM, VMEM, VMEM],
        out_specs=VMEM,
        out_shape=jax.ShapeDtypeStruct((128, 2, 1024), F32),
        scratch_shapes=[pltpu.VMEM(terms.shape, BF16), pltpu.SemaphoreType.DMA((2,))],
        compiler_params=params(10),
        cost_estimate=cost(1 << 28, 1 << 22),
        name="finish",
    )(place, terms, base, order)


def weight_kernel(place_ref, *refs):
    blocks, out_ref, rows = refs[:N_TM], refs[N_TM], refs[-1]
    own, far, z = place_ref[1], place_ref[2], place_ref[3]
    for k in range(N_TM):
        source = (z - (own ^ k)) & 7
        for dx in (0, 1):
            chip = (far ^ dx) * 8 + source
            for dc in (0, 1):
                early = pl.multiple_of(dc * SIDE_A + chip * FIRST, 8)
                late = pl.multiple_of(COLS_A + chip * 2 * SECOND + dc * SECOND, 8)
                for p in (0, 1):
                    block = blocks[k][dc, dx, p].astype(F32)
                    rows[p, pl.ds(early, FIRST), :] = block[:FIRST]
                    rows[p, pl.ds(late, SECOND), :] = block[FIRST:]
    for p in (0, 1):
        flipped = rows[p].T
        straight = flipped.astype(BF16)
        out_ref[:256, 1024 * p : 1024 * p + 1024] = (-flipped).astype(BF16) if p else straight
        out_ref[256:, 1024 * (1 - p) : 1024 * (1 - p) + 1024] = straight


def weight_stack(place, blocks):
    return pl.pallas_call(
        weight_kernel,
        in_specs=[SMEM] + [VMEM] * N_TM,
        out_specs=VMEM,
        out_shape=jax.ShapeDtypeStruct((HALF, 2048), BF16),
        scratch_shapes=[pltpu.VMEM((2, 1024, 256), F32)],
        compiler_params=params(10),
        cost_estimate=cost(1 << 27, 1 << 22),
        name="weights",
    )(place, *blocks)


def beam_kernel(kept_ref, swapped_ref, second_ref, weight_ref, out_ref):
    total = None
    for p in (0, 1):
        lanes = slice(HALF * p, HALF * p + HALF)
        column = 1024 * p
        for ref in (kept_ref, swapped_ref, second_ref):
            count = ref.shape[0]
            term = dot_nn(weight_ref[:, column : column + count], ref[:, lanes])
            column += count
            total = term if total is None else total + term
    out_ref[...] = total.T.astype(BF16)


def beam_sum(kept, swapped, second, weights):
    return pl.pallas_call(
        beam_kernel,
        in_specs=[VMEM] * 4,
        out_specs=VMEM,
        out_shape=jax.ShapeDtypeStruct((HALF, HALF), BF16),
        compiler_params=params(10),
        cost_estimate=cost(1 << 29, 1 << 22),
        name="beams",
    )(kept, swapped, second, weights)


def swap(array, axis):
    return lax.ppermute(array, axis, [(0, 1), (1, 0)])


def with_partners(array):
    pairs = lambda k: [(i, i ^ k) for i in range(N_TM)]
    return [array] + [lax.ppermute(array, TM, pairs(k)) for k in range(1, N_TM)]


def to_partners(arrays):
    pairs = lambda k: [(i, i ^ k) for i in range(N_TM)]
    return [arrays[0]] + [lax.ppermute(arrays[k], TM, pairs(k)) for k in range(1, N_TM)]


def behind(value, other):
    return lax.optimization_barrier((value, other))[0]


def step(voltages, beam_weights):
    left, cosine, sine, right = dft_tables()
    tables = (jnp.asarray(left, BF16), jnp.asarray(np.stack([cosine, sine])), jnp.asarray(right, BF16))
    signal = voltages.reshape(2, 32, SPECTRA, 32, 128).transpose(0, 1, 3, 2, 4)
    signal = signal.reshape(2, 32, 128, 128)
    where = ("stat_2", TM, "stat_0", "stat_1")
    place = jnp.stack([lax.axis_index(a) for a in where]).astype(jnp.int32)

    spots = [(x, z, t) for x in (0, 1) for z in range(8) for t in range(N_TM)]
    at = lambda x, z, t: (x * 8 + z % 8) * N_TM + t
    rings = [[(at(x, z, t), at(x ^ dx, z + t, t)) for x, z, t in spots] for dx in (0, 1)]
    block = jnp.stack([lax.ppermute(beam_weights, (*CHIP, *TM), ring) for ring in rings])

    (ready_a,) = dft_part(place, signal, tables, FIRST, True)
    own_b, other_b = dft_part(place, signal, tables, SECOND, False)
    partner_b = swap(other_b, "stat_2")
    ready_b = jnp.concatenate([own_b, partner_b], 1)

    near = swap(block, "stat_2")
    block = jnp.stack([block, near])
    blocks_k = with_partners(block)
    columns = natural_columns(behind(lax.axis_index("stat_2"), ready_b))
    order = (columns[:, None] == jnp.arange(1024, dtype=jnp.int32)[None, :]).astype(BF16)

    arrived = lax.all_to_all(ready_a, CHIP, 0, 0, tiled=True)
    second = lax.all_to_all(ready_b, CHIP, 0, 0, tiled=True).reshape(COLS_B, 1024)
    kept = arrived[:, 0].reshape(SIDE_A, 1024)
    other = arrived[:, 1].reshape(SIDE_A, 1024)
    swapped = swap(other, "stat_2")
    terms = gram_first(place, kept, swapped)
    terms = to_partners(terms)
    blocks = gram_second(second, kept, swapped)
    last = lax.all_to_all(blocks, TM, 0, 0, tiled=True)

    weights = weight_stack(place, blocks_k)
    beams = beam_sum(kept, swapped, second, weights)
    beams = beams.reshape(NF // 32, SPECTRA, 2, 256)
    base = spread_first(terms, order)
    rows = finish(place, last, base, order)
    return beams, rows[:, None]


def solution(mesh):
    finer = Mesh(
        mesh.devices.reshape(2, 8, 2, 4, 2), ("stat_0", "stat_1", "stat_2", "tm_0", "tm_1")
    )
    return jax.shard_map(
        step,
        mesh=finer,
        in_specs=(P(None, STAT, TM, None), P(None, STAT, None)),
        out_specs=(P(STAT, TM, None, None), P(TM, STAT, None, None)),
        check_vma=False,
    )
```
